8 devices in a mesh: dp: 2 (over z, y), ep: 4 (over x, core).
Axes of the slice: x: 2, y: 2, z: 1, core: 2. Of those that a mesh axis runs over, the one named last changes fastest.
Arguments:
- h0: bfloat16 [8, 128, 2048], P(('dp', 'ep')), parts along dimension 0
- idx: int32 [8, 128, 8], P(('dp', 'ep')), parts along dimension 0
- slot: int32 [8, 128, 8], P(('dp', 'ep')), parts along dimension 0
- norm_attn: bfloat16 [2048], replicated
- wq: bfloat16 [2048, 4096], replicated
- wk: bfloat16 [2048, 512], replicated
- wv: bfloat16 [2048, 512], replicated
- wo: bfloat16 [4096, 2048], replicated
- norm_ffn: bfloat16 [2048], replicated
- w1: bfloat16 [2048, 6144], replicated
- w3: bfloat16 [2048, 6144], replicated
- w2: bfloat16 [6144, 2048], replicated
- norm_moe: bfloat16 [2048], replicated
- wr: bfloat16 [2048, 128], replicated
- ue1: bfloat16 [128, 2048, 768], P('ep')
- ue3: bfloat16 [128, 2048, 768], P('ep')
- ue2: bfloat16 [128, 768, 2048], P('ep')
Outputs:
- output: bfloat16 [8, 128, 2048], P(('dp', 'ep')), parts along dimension 0
There are 2 independent parts. The reference program is written for one: setup_inputs(seed, part) draws one part's arguments, and reference() takes and returns one part's arrays. A program takes and returns all parts, laid end to end along the dimension named above; an argument that names none is the same for every part.
All inputs are finite; a program needn't handle non-finite values.
Results may differ from the reference program's by a relative error of at most 0.0127889.
Values are sent between devices in bfloat16 or wider.
A program may use at most 1.75 GiB of HBM per device.

```python
import jax
import jax.numpy as jnp
from jax import lax

D = 2048
HEADS = 32
KV_HEADS = 4
HEAD = 128
FF = 6144
EXPERTS = 128
TOP = 8
FE = 768
SEQS_DEV = 1
SEQ = 128
EP = 4

TOKENS = SEQS_DEV * SEQ
CAP = 2 * TOKENS * TOP // EXPERTS
EPS = 1e-6
ROPE_BASE = 10000.0


def _w(key, shape, fan_in, scale=1.0):
    return (scale * fan_in ** -0.5 * jax.random.normal(key, shape, jnp.float32)).astype(jnp.bfloat16)


def _perms(key, count, size):
    return jax.vmap(lambda k: jax.random.permutation(k, size))(jax.random.split(key, count))


def setup_inputs(seed: int = 0, part: int = 0) -> dict:
    key = jax.random.PRNGKey(seed)
    ks = jax.random.split(key, 14)
    kp = jax.random.split(jax.random.fold_in(key, part), 4)
    kd = jax.random.split(jax.random.fold_in(jax.random.fold_in(key, part), 7), 4)
    avg = TOKENS * TOP // EXPERTS
    c = jnp.arange(TOKENS * TOP).reshape(TOKENS, TOP)
    half = TOKENS * TOP // 2
    low = c < half
    e0 = jnp.where(low, c % EXPERTS, (c - half) % (EXPERTS // 2))
    s0 = jnp.where(low, c // EXPERTS, avg // 2 + (c - half) // (EXPERTS // 2))
    shift = jax.random.randint(kd[2], (EP, EXPERTS), 0, CAP)
    tperm = jnp.broadcast_to(_perms(kd[3], EP, TOKENS)[:, :, None], (EP, TOKENS, TOP))
    idx = jnp.take_along_axis(jnp.broadcast_to(e0, (EP, TOKENS, TOP)), tperm, axis=1)
    slot = jnp.take_along_axis((s0[None] + shift[:, e0]) % CAP, tperm, axis=1)
    rshape = (EP * SEQS_DEV, SEQ, TOP)

    def nrm(k):
        return (1.0 + 0.2 * jax.random.normal(k, (D,), jnp.float32)).astype(jnp.bfloat16)

    return {
        'h0': jax.random.normal(kp[0], (EP * SEQS_DEV, SEQ, D), jnp.float32).astype(jnp.bfloat16),
        'idx': idx.reshape(rshape).astype(jnp.int32),
        'slot': slot.reshape(rshape).astype(jnp.int32),
        'norm_attn': nrm(ks[0]),
        'wq': _w(ks[1], (D, HEADS * HEAD), D),
        'wk': _w(ks[2], (D, KV_HEADS * HEAD), D),
        'wv': _w(ks[3], (D, KV_HEADS * HEAD), D),
        'wo': _w(ks[4], (HEADS * HEAD, D), HEADS * HEAD, 2.0),
        'norm_ffn': nrm(ks[5]),
        'w1': _w(ks[6], (D, FF), D),
        'w3': _w(ks[7], (D, FF), D),
        'w2': _w(ks[8], (FF, D), FF, 2.0),
        'norm_moe': nrm(ks[9]),
        'wr': _w(ks[10], (D, EXPERTS), D, 2.0),
        'ue1': _w(ks[11], (EXPERTS, D, FE), D),
        'ue3': _w(ks[12], (EXPERTS, D, FE), D),
        'ue2': _w(ks[13], (EXPERTS, FE, D), FE, 2.0),
    }


def _rms(x, w):
    xf = x.astype(jnp.float32)
    r = lax.rsqrt(jnp.mean(xf * xf, axis=-1, keepdims=True) + EPS)
    return (xf * r * w.astype(jnp.float32)).astype(jnp.bfloat16)


def _rope(x, cos, sin):
    h = HEAD // 2
    x1 = x[..., :h]
    x2 = x[..., h:]
    return jnp.concatenate([x1 * cos - x2 * sin, x2 * cos + x1 * sin], axis=-1)


def _dense_seq(h, na, wq, wk, wv, wo, nf, w1, w3, w2):
    f32 = jnp.float32
    bf = jnp.bfloat16
    pos = jnp.arange(SEQ).astype(f32)
    inv = ROPE_BASE ** (-2.0 * jnp.arange(HEAD // 2).astype(f32) / HEAD)
    ang = pos[:, None] * inv[None, :]
    cos = jnp.cos(ang)[:, None, :]
    sin = jnp.sin(ang)[:, None, :]
    x = _rms(h, na)
    q = _rope(jnp.dot(x, wq, preferred_element_type=f32).reshape(SEQ, HEADS, HEAD), cos, sin).astype(bf)
    k = _rope(jnp.dot(x, wk, preferred_element_type=f32).reshape(SEQ, KV_HEADS, HEAD), cos, sin).astype(bf)
    v = jnp.dot(x, wv, preferred_element_type=f32).astype(bf).reshape(SEQ, KV_HEADS, HEAD)
    q = q.reshape(SEQ, KV_HEADS, HEADS // KV_HEADS, HEAD)
    s = jnp.einsum('qgrd,kgd->grqk', q.astype(f32), k.astype(f32)) * HEAD ** -0.5
    causal = jnp.arange(SEQ)[:, None] >= jnp.arange(SEQ)[None, :]
    s = jnp.where(causal, s, -jnp.inf)
    p = jax.nn.softmax(s, axis=-1).astype(bf)
    o = jnp.einsum('grqk,kgd->qgrd', p.astype(f32), v.astype(f32)).astype(bf).reshape(SEQ, HEADS * HEAD)
    a = (h.astype(f32) + jnp.dot(o, wo, preferred_element_type=f32)).astype(bf)
    z = _rms(a, nf)
    hid = (jax.nn.silu(jnp.dot(z, w1, preferred_element_type=f32)) * jnp.dot(z, w3, preferred_element_type=f32)).astype(bf)
    return a.astype(f32) + jnp.dot(hid, w2, preferred_element_type=f32)


def reference(h0, idx, slot, norm_attn, wq, wk, wv, wo, norm_ffn, w1, w3, w2, norm_moe, wr, ue1, ue3, ue2):
    f32 = jnp.float32
    bf = jnp.bfloat16
    n = EP * TOKENS
    ix = idx.reshape(n, TOP)
    sl = slot.reshape(n, TOP)
    u = _rms(h0.reshape(n, D), norm_moe)
    logits = jnp.dot(u, wr, preferred_element_type=f32)
    g = jax.nn.softmax(jnp.take_along_axis(logits, ix, axis=1), axis=-1)
    rows = jnp.broadcast_to(jnp.arange(n, dtype=jnp.int32)[:, None], (n, TOP))
    src = rows // TOKENS
    tok = jnp.full((EP, EXPERTS, CAP), n, jnp.int32).at[src, ix, sl].set(rows)
    gb = jnp.zeros((EP, EXPERTS, CAP), f32).at[src, ix, sl].set(g)
    tok = tok.transpose(1, 0, 2).reshape(EXPERTS, EP * CAP)
    x = jnp.take(u, tok, axis=0, mode='fill', fill_value=0)

    def expert(args):
        xe, e1, e3, e2 = args
        hid = (jax.nn.silu(jnp.dot(xe, e1, preferred_element_type=f32)) * jnp.dot(xe, e3, preferred_element_type=f32)).astype(bf)
        return jnp.dot(hid, e2, preferred_element_type=f32).astype(bf)

    y = lax.map(expert, (x, ue1, ue3, ue2))
    gw = gb.transpose(1, 0, 2).reshape(EXPERTS, EP * CAP, 1)
    m = jnp.zeros((n, D), f32).at[tok.reshape(-1)].add((gw * y.astype(f32)).reshape(-1, D), mode='drop')
    dense = lax.map(lambda hs: _dense_seq(hs, norm_attn, wq, wk, wv, wo, norm_ffn, w1, w3, w2), h0)
    return (dense + m.reshape(EP * SEQS_DEV, SEQ, D)).astype(bf)
```

```python
import functools

import jax
import jax.numpy as jnp
import numpy as np
from jax import lax
from jax.experimental import pallas as pl
from jax.experimental.pallas import tpu as pltpu
from jax.sharding import PartitionSpec as P

MESH = pl.DeviceIdType.MESH
HEAD = 128
EPS = 1e-6
ROPE_BASE = 10000.0

T, D, FE, FF, TOP, CAP = 128, 2048, 768, 6144, 8, 16
EL = 16
QT = 512
CW = 512
NC = D // CW
HW = CW // 2
NA = 4
NB = 4
NQ = 8
NF = FF // FE
N1 = 4
A_FF1 = 2 + NQ
A_EXP = A_FF1 + 2 * N1
A_FF2 = A_EXP + 2 * EL
A_END = A_FF2 + 2 * (NF - N1)
B_EXP = 8
B_W2 = B_EXP + 4 * NC
B_END = B_W2 + 8

f32, bf16 = jnp.float32, jnp.bfloat16


def _dot(a, b):
    return jnp.dot(a, b, preferred_element_type=f32)


def _kernel(h0, idx, slot, na, nf, nm, cos, sin, wr, wq, wk, wv, wo, w1, w3, w2, ue1, ue3, ue2, out,
            xz, ar, fs, u, info, ws, x, kk, vv, g, pp, rc, r1, r2, ra, rb,
            sem_a, sem_b, send, recv):
    dp, ep = lax.axis_index('dp'), lax.axis_index('ep')
    px = (dp, lax.rem(ep + 2, 4))
    py = (1 - dp, ep)
    pd = (1 - dp, lax.rem(ep + 2, 4))
    pc = (dp, ep + 1 - 2 * lax.rem(ep, 2))
    e0 = dp * EL

    def a_copy(kind, i, s):
        if kind == 'k':
            return pltpu.make_async_copy(wk, ra.at[s, :, pl.ds(0, QT)], sem_a.at[s])
        if kind == 'v':
            return pltpu.make_async_copy(wv, ra.at[s, :, pl.ds(0, QT)], sem_a.at[s])
        if kind == 'q':
            c = pl.multiple_of(i * QT, QT)
            return pltpu.make_async_copy(wq.at[:, pl.ds(c, QT)], ra.at[s, :, pl.ds(0, QT)], sem_a.at[s])
        if kind in ('w1', 'w3'):
            c = pl.multiple_of(i * FE, FE)
            return pltpu.make_async_copy((w1 if kind == 'w1' else w3).at[:, pl.ds(c, FE)], ra.at[s], sem_a.at[s])
        return pltpu.make_async_copy((ue1 if kind == 'e1' else ue3).at[e0 + i], ra.at[s], sem_a.at[s])

    def a_start(t, lo, hi):
        s = lax.rem(t, NA)

        def pairs(first, last, names, base):
            a, b = max(first, lo), min(last, hi)
            if a >= b:
                return
            for par in (0, 1):
                @pl.when((t >= a) & (t < b) & (lax.rem(t - first, 2) == par))
                def _():
                    a_copy(names[par], base + (t - first) // 2, s).start()

        if lo < A_FF1:
            @pl.when(t < A_FF1)
            def _():
                a_copy('q', t - 2, s).start()
        pairs(A_FF1, A_EXP, ('w1', 'w3'), 0)
        pairs(A_EXP, A_FF2, ('e1', 'e3'), 0)
        pairs(A_FF2, A_END, ('w1', 'w3'), N1)

    def b_copy(kind, i, s):
        if kind == 'wo':
            return pltpu.make_async_copy(
                wo.at[pl.ds(lax.rem(i, 2) * 4, 4), :, pl.ds(pl.multiple_of((i // 2) * CW, CW), CW)],
                rb.at[s, :, pl.ds(0, QT), :], sem_b.at[s])
        if kind == 'w2':
            return pltpu.make_async_copy(
                w2.at[pl.ds(lax.rem(i, 2) * 4, 4), :, pl.ds(pl.multiple_of((i // 2) * CW, CW), CW)],
                rb.at[s], sem_b.at[s])
        return pltpu.make_async_copy(
            ue2.at[pl.ds(e0 + lax.rem(i, 4) * 4, 4), :, pl.ds(pl.multiple_of((i // 4) * CW, CW), CW)],
            rb.at[s], sem_b.at[s])

    def b_start(t, lo, hi):
        s = lax.rem(t, NB)
        for first, last, name in ((0, B_EXP, 'wo'), (B_EXP, B_W2, 'e2'), (B_W2, B_END, 'w2')):
            a, b = max(first, lo), min(last, hi)
            if a >= b:
                continue

            @pl.when((t >= a) & (t < b))
            def _():
                b_copy(name, t - first, s).start()

    specs = {}

    def rdma(key, src, dst, to):
        i = specs.setdefault(key, len(specs))
        return pltpu.make_async_remote_copy(src_ref=src, dst_ref=dst, send_sem=send.at[i], recv_sem=recv.at[i],
                                            device_id=to, device_id_type=MESH)

    ag = {
        'ix': lambda: rdma('ix', info.at[0], info.at[2], px),
        'iy': lambda: rdma('iy', info.at[0], info.at[3], py),
        'id': lambda: rdma('id', info.at[0], info.at[6], pd),
        'ic': lambda: rdma('ic', info.at[0], info.at[1], pc),
        'x0': lambda: rdma('x0', u.at[0, 0], u.at[2, 0], px),
        'x1': lambda: rdma('x1', u.at[0, 1], u.at[2, 1], px),
        'y1': lambda: rdma('y1', u.at[0, 1], u.at[3, 1], py),
        'y0': lambda: rdma('y0', u.at[0, 0], u.at[3, 0], py),
        'c': lambda: rdma('c', u.at[0], u.at[1], pc),
        'd0': lambda: rdma('d0', u.at[2, 0], u.at[6, 0], py),
        'd1': lambda: rdma('d1', u.at[3, 1], u.at[6, 1], px),
        'cx': lambda: rdma('cx', u.at[2], u.at[4], pc),
        'cy': lambda: rdma('cy', u.at[3], u.at[5], pc),
        'cd': lambda: rdma('cd', u.at[6], u.at[7], pc),
        'icx': lambda: rdma('icx', info.at[2], info.at[4], pc),
        'icy': lambda: rdma('icy', info.at[3], info.at[5], pc),
        'icd': lambda: rdma('icd', info.at[6], info.at[7], pc),
    }
    for key in ag:
        specs.setdefault(key, len(specs))

    def rs(name, c):
        key = (name, c)
        if name == 'c':
            return rdma(key, pp.at[c, pl.ds(4, 4)], rc.at[c], pc)
        if name == 'xa':
            return rdma(key, pp.at[c, 1, 0], r1.at[c, 0], px)
        if name == 'xb':
            return rdma(key, pp.at[c, 3, 0], r1.at[c, 1], px)
        if name == 'ya':
            return rdma(key, pp.at[c, 2, 1], r1.at[c, 2], py)
        if name == 'yb':
            return rdma(key, pp.at[c, 3, 1], r1.at[c, 3], py)
        if name == 'y2':
            return rdma(key, pp.at[c, 2, 0], r2.at[c, 0], py)
        return rdma(key, pp.at[c, 1, 1], r2.at[c, 1], px)

    def rs_core(c):
        rs('c', c).start()

    def rs_first(c):
        rs('c', c).wait_recv()
        for q in (3, 1, 2, 0):
            pp[c, q] = pp[c, q] + rc[c, q]
        for name in ('xb', 'yb', 'xa', 'ya'):
            rs(name, c).start()

    def rs_second(c):
        rs('xb', c).wait_recv()
        pp[c, 2, 0] = pp[c, 2, 0] + r1[c, 1]
        rs('y2', c).start()
        rs('yb', c).wait_recv()
        pp[c, 1, 1] = pp[c, 1, 1] + r1[c, 3]
        rs('x2', c).start()

    def rs_last(c):
        lo = slice(c * CW, c * CW + HW)
        hi = slice(c * CW + HW, (c + 1) * CW)
        rs('xa', c).wait_recv()
        rs('y2', c).wait_recv()
        out[0, :, lo] = (fs[:, lo] + ((pp[c, 0, 0] + r1[c, 0]) + r2[c, 0])).astype(bf16)
        rs('ya', c).wait_recv()
        rs('x2', c).wait_recv()
        out[0, :, hi] = (fs[:, hi] + ((pp[c, 0, 1] + r1[c, 2]) + r2[c, 1])).astype(bf16)

    barrier = pltpu.get_barrier_semaphore()
    for to in (px, py, pd, pc):
        pl.semaphore_signal(barrier, inc=1, device_id=to, device_id_type=MESH)
    a_copy('k', 0, 0).start()
    a_copy('v', 0, 1).start()
    for i in range(NA - 2):
        a_copy('q', i, 2 + i).start()
    for i in range(NB):
        b_copy('wo', i, i).start()

    def norms(i, _):
        rows = pl.ds(pl.multiple_of(i * 16, 16), 16)
        xf = h0[0, rows, :].astype(f32)
        xr = xf * lax.rsqrt(jnp.mean(xf * xf, axis=-1, keepdims=True) + EPS)
        un = (xr * nm[...].astype(f32)).astype(bf16)
        u[0, 0, rows, :] = un[:, :D // 2]
        u[0, 1, rows, :] = un[:, D // 2:]
        xz[rows, :] = (xr * na[...].astype(f32)).astype(bf16)
        return 0

    lax.fori_loop(0, T // 16, norms, 0)
    pl.semaphore_wait(barrier, 4)
    for key in ('x0', 'y1', 'c', 'x1', 'y0'):
        ag[key]().start()

    logits = _dot(u[0, 0], wr[pl.ds(0, D // 2), :]) + _dot(u[0, 1], wr[pl.ds(D // 2, D // 2), :])
    lt = logits.T
    idt = idx[0].astype(f32).T
    slt = slot[0].astype(f32).T
    ex = lax.broadcasted_iota(jnp.int32, (T, T), 0).astype(f32)
    sel = jnp.concatenate(
        [jnp.sum(jnp.where(ex == idt[j:j + 1, :], lt, 0.0), axis=0, keepdims=True) for j in range(TOP)], axis=0)
    gate = jnp.exp(sel - jnp.max(sel, axis=0, keepdims=True))
    gate = gate / jnp.sum(gate, axis=0, keepdims=True)
    info[0, pl.ds(0, TOP), :] = idt * float(CAP) + slt
    info[0, pl.ds(TOP, TOP), :] = gate

    cs, sn = cos[...], sin[...]

    def rope(v):
        return (v * cs + pltpu.roll(v, HEAD // 2, 1) * sn).astype(bf16)

    a_copy('k', 0, 0).wait()
    kf = _dot(xz[...], ra[0, :, pl.ds(0, QT)])
    a_copy('q', 2, 0).start()
    for n in range(4):
        kk[n] = rope(kf[:, n * HEAD:(n + 1) * HEAD])
    for key in ('ix', 'iy', 'id', 'ic'):
        ag[key]().start()
    a_copy('v', 0, 1).wait()
    vf = _dot(xz[...], ra[1, :, pl.ds(0, QT)])
    a_copy('q', 3, 1).start()
    for n in range(4):
        vv[n] = vf[:, n * HEAD:(n + 1) * HEAD].astype(bf16)
    causal = lax.broadcasted_iota(jnp.int32, (T, T), 0) >= lax.broadcasted_iota(jnp.int32, (T, T), 1)

    def q_step(i, _):
        t = 2 + i
        s = lax.rem(t, NA)
        a_copy('q', i, s).wait()
        qf = _dot(xz[...], ra[s, :, pl.ds(0, QT)])
        a_start(t + NA, 2 + NA, A_FF1 + NA)
        kg, vg = kk[i // 2], vv[i // 2]
        for n in range(4):
            qh = rope(qf[:, n * HEAD:(n + 1) * HEAD])
            sc = lax.dot_general(qh, kg, (((1,), (1,)), ((), ())), preferred_element_type=f32) * HEAD ** -0.5
            sc = jnp.where(causal, sc, -jnp.inf)
            p = jnp.exp(sc - jnp.max(sc, axis=-1, keepdims=True))
            p = (p * (1.0 / jnp.sum(p, axis=-1, keepdims=True))).astype(bf16)
            g[i, :, n * HEAD:(n + 1) * HEAD] = _dot(p, vg).astype(bf16)
        return 0

    lax.fori_loop(0, NQ, q_step, 0)

    ag['x0']().wait_recv()
    ag['d0']().start()
    ag['y1']().wait_recv()
    ag['d1']().start()

    def wo_step(n, _):
        cols = pl.ds(pl.multiple_of(n * CW, CW), CW)
        acc = h0[0, :, cols].astype(f32)
        prod = None
        for half in range(2):
            t = 2 * n + half
            s = lax.rem(t, NB)
            b_copy('wo', t, s).wait()
            for i in range(4):
                term = _dot(g[half * 4 + i, :, pl.ds(0, QT)], rb[s, i, pl.ds(0, QT), :])
                prod = term if prod is None else prod + term
            b_start(t + NB, NB, B_EXP + NB)
        ar[:, cols] = (acc + prod).astype(bf16)
        return 0

    lax.fori_loop(0, D // CW, wo_step, 0)

    def znorm(i, _):
        rows = pl.ds(pl.multiple_of(i * 16, 16), 16)
        xf = ar[rows, :].astype(f32)
        xr = xf * lax.rsqrt(jnp.mean(xf * xf, axis=-1, keepdims=True) + EPS)
        xz[rows, :] = (xr * nf[...].astype(f32)).astype(bf16)
        return 0

    lax.fori_loop(0, T // 16, znorm, 0)

    for key in ('ix', 'iy', 'id', 'x1', 'y0'):
        ag[key]().wait_recv()
    for key in ('icx', 'icy', 'icd', 'cx', 'cy'):
        ag[key]().start()

    def gated(lhs, t, kinds, i, hi):
        s1, s3 = lax.rem(t, NA), lax.rem(t + 1, NA)
        a_copy(kinds[0], i, s1).wait()
        h1 = _dot(lhs, ra[s1])
        a_copy(kinds[1], i, s3).wait()
        h3 = _dot(lhs, ra[s3])
        for k in (0, 1):
            a_start(t + NA + k, *hi)
        return (h1 * jax.nn.sigmoid(h1) * h3).astype(bf16)

    def ffn1(i, _):
        g[i] = gated(xz[...], A_FF1 + 2 * i, ('w1', 'w3'), i, (A_FF1 + NA, A_EXP + NA))
        return 0

    lax.fori_loop(0, N1, ffn1, 0)

    base = ((ep * 32 + e0) * CAP).astype(f32)

    def build(r, _):
        for half in range(2):
            row = lax.broadcasted_iota(jnp.int32, (T, T), 0).astype(f32) + (base + float(half * T))
            w = jnp.zeros((T, T), f32)
            d = jnp.zeros((T, T), f32)
            for j in range(TOP):
                hit = row == info[r, pl.ds(j, 1), :]
                w = jnp.where(hit, info[r, pl.ds(TOP + j, 1), :], w)
                d = jnp.where(hit, 1.0, d)
            wt = w.T
            hi = wt.astype(bf16)
            rest = wt - hi.astype(f32)
            mid = rest.astype(bf16)
            low = (rest - mid.astype(f32)).astype(bf16)
            for n, part in enumerate((hi, mid, low)):
                ws[r, pl.ds(n * T, T), half * T:(half + 1) * T] = part
            db = d.astype(bf16)
            for c in range(4):
                rows = _dot(db, u[r, c // 2, :, (c % 2) * 512:(c % 2 + 1) * 512]).astype(bf16)
                x[pl.ds(half * 8, 8), pl.ds(pl.multiple_of(r * CAP, CAP), CAP), c * 512:(c + 1) * 512] = (
                    rows.reshape(8, CAP, 512))
        return 0

    for key in ('d0', 'd1'):
        ag[key]().wait_recv()
    ag['cd']().start()
    for key in ('ic', 'icx', 'icy', 'icd', 'c', 'cx', 'cy', 'cd'):
        ag[key]().wait_recv()
    lax.fori_loop(0, 8, build, 0)

    def experts(e, _):
        x[e, :, :FE] = gated(x[e], A_EXP + 2 * e, ('e1', 'e3'), e, (A_EXP + NA, A_FF2 + NA))
        return 0

    lax.fori_loop(0, EL, experts, 0)

    YC = 1024

    def chunk(c):
        def part(k, _):
            t = B_EXP + 4 * c + k
            s = lax.rem(t, NB)
            b_copy('e2', 4 * c + k, s).wait()
            for i in range(4):
                x[4 * k + i, :, YC:YC + CW] = _dot(x[4 * k + i, :, :FE], rb[s, i]).astype(bf16)
            b_start(t + NB, B_EXP + NB, B_W2 + NB)
            return 0

        if c == 0:
            lax.fori_loop(0, 4, part, 0)
        else:
            lax.fori_loop(0, 2, part, 0)
            rs_first(c - 1)
            lax.fori_loop(2, 4, part, 0)

        def combine(q, _):
            core, yy, xx = q // 4, lax.rem(q // 2, 2), lax.rem(q, 2)
            r = jnp.where(xx * yy == 1, 6 + core, jnp.where(xx + yy == 0, core, 1 + xx + 2 * yy + 2 * core))
            yr = x[:, pl.ds(pl.multiple_of(r * CAP, CAP), CAP), YC:YC + CW].reshape(2 * T, CW)
            three = _dot(ws[r], yr)
            m = (three[:T] + three[T:2 * T]) + three[2 * T:]
            pp[c, q, 0] = m[:, :HW]
            pp[c, q, 1] = m[:, HW:]
            return 0

        lax.fori_loop(0, 8, combine, 0)
        rs_core(c)

    for c in range(NC):
        chunk(c)

    def ffn2(i, _):
        g[i] = gated(xz[...], A_FF2 - 2 * N1 + 2 * i, ('w1', 'w3'), i, (A_FF2 + NA, A_END))
        for at, fn in ((N1, lambda: rs_second(0)), (N1 + 1, lambda: rs_first(NC - 1)), (N1 + 3, lambda: rs_second(1))):
            @pl.when(i == at)
            def _():
                fn()
        return 0

    lax.fori_loop(N1, NF, ffn2, 0)

    def w2_step(n, _):
        cols = pl.ds(pl.multiple_of(n * CW, CW), CW)
        prod = None
        for half in range(2):
            t = B_W2 + 2 * n + half
            s = lax.rem(t, NB)
            b_copy('w2', 2 * n + half, s).wait()
            for i in range(4):
                term = _dot(g[half * 4 + i], rb[s, i])
                prod = term if prod is None else prod + term
            b_start(t + NB, B_W2 + NB, B_END)
        fs[:, cols] = ar[:, cols].astype(f32) + prod
        return 0

    lax.fori_loop(0, 2, w2_step, 0)
    rs_second(2)
    lax.fori_loop(2, 4, w2_step, 0)
    rs_second(3)
    for c in range(NC):
        rs_last(c)
    for key in ag:
        ag[key]().wait_send()
    for c in range(NC):
        for name in ('c', 'xa', 'xb', 'ya', 'yb', 'y2', 'x2'):
            rs(name, c).wait_send()


def solution(mesh):
    ang = (np.arange(T, dtype=np.float32)[:, None]
           * (ROPE_BASE ** (-2.0 * np.arange(HEAD // 2) / HEAD)).astype(np.float32)[None, :])
    cos = np.cos(ang.astype(np.float64)).astype(np.float32)
    sin = np.sin(ang.astype(np.float64)).astype(np.float32)
    cos2 = np.concatenate([cos, cos], axis=1)
    sin2 = np.concatenate([-sin, sin], axis=1)
    ncopies = 17 + 7 * NC

    def local(h0, idx, slot, na, wq, wk, wv, wo, nf, w1, w3, w2, nm, wr, ue1, ue3, ue2):
        vm = pl.BlockSpec(memory_space=pltpu.VMEM)
        hb = pl.BlockSpec(memory_space=pl.ANY)
        return pl.pallas_call(
            _kernel,
            out_shape=jax.ShapeDtypeStruct(h0.shape, bf16),
            in_specs=[vm] * 9 + [hb] * 10,
            out_specs=vm,
            scratch_shapes=[
                pltpu.VMEM((T, D), bf16),
                pltpu.VMEM((T, D), bf16),
                pltpu.VMEM((T, D), f32),
                pltpu.VMEM((8, 2, T, D // 2), bf16),
                pltpu.VMEM((8, 2 * TOP, T), f32),
                pltpu.VMEM((8, 3 * T, 2 * T), bf16),
                pltpu.VMEM((EL, T, D), bf16),
                pltpu.VMEM((4, T, HEAD), bf16),
                pltpu.VMEM((4, T, HEAD), bf16),
                pltpu.VMEM((NF, T, FE), bf16),
                pltpu.VMEM((NC, 8, 2, T, HW), f32),
                pltpu.VMEM((NC, 4, 2, T, HW), f32),
                pltpu.VMEM((NC, 4, T, HW), f32),
                pltpu.VMEM((NC, 2, T, HW), f32),
                pltpu.VMEM((NA, D, FE), bf16),
                pltpu.VMEM((NB, 4, FE, CW), bf16),
                pltpu.SemaphoreType.DMA((NA,)),
                pltpu.SemaphoreType.DMA((NB,)),
                pltpu.SemaphoreType.DMA((ncopies,)),
                pltpu.SemaphoreType.DMA((ncopies,)),
            ],
            compiler_params=pltpu.CompilerParams(collective_id=0, has_side_effects=True,
                                                 vmem_limit_bytes=67043328),
            name='scmoe',
        )(h0, idx, slot, na.reshape(1, D), nf.reshape(1, D), nm.reshape(1, D),
          jnp.asarray(cos2), jnp.asarray(sin2), wr, wq, wk, wv, wo.reshape(8, QT, D),
          w1, w3, w2.reshape(8, FE, D), ue1, ue3, ue2)

    rows = P(('dp', 'ep'))
    in_specs = (rows,) * 3 + (P(),) * 11 + (P('ep'),) * 3
    return jax.shard_map(local, mesh=mesh, in_specs=in_specs, out_specs=rows, check_vma=False)
```

```python
import functools

import jax
import jax.numpy as jnp
import numpy as np
from jax import lax
from jax.experimental import pallas as pl
from jax.experimental.pallas import tpu as pltpu
from jax.sharding import PartitionSpec as P

MESH = pl.DeviceIdType.MESH
HEAD = 128
EPS = 1e-6
ROPE_BASE = 10000.0

T, D, FE, FF, TOP, CAP = 128, 2048, 768, 6144, 8, 16
EL = 16
QT = 512
CW = 512
NC = D // CW
HW = CW // 2
NA = 4
NB = 4
NQ = 8
Q_FWD = 2
PLACE = (0, 2, 3, 6, 1, 4, 5, 7)
NF = FF // FE
N1 = 1
A_FF1 = 2 + NQ
A_EXP = A_FF1 + 2 * N1
A_FF2 = A_EXP + 2 * EL
A_END = A_FF2 + 2 * (NF - N1)
B_EXP = 8
B_W2 = B_EXP + 4 * NC
B_END = B_W2 + 8

f32, bf16 = jnp.float32, jnp.bfloat16


def _dot(a, b):
    return jnp.dot(a, b, preferred_element_type=f32)


def _kernel(h0, idx, slot, na, nf, nm, cos, sin, wr, wq, wk, wv, wo, w1, w3, w2, ue1, ue3, ue2, out,
            xz, ar, fs, qa, qb, u, info, ws, x, kk, vv, g, pp, rc, r1, r2, ra, rb,
            sem_a, sem_b, send, recv):
    dp, ep = lax.axis_index('dp'), lax.axis_index('ep')
    px = (dp, lax.rem(ep + 2, 4))
    py = (1 - dp, ep)
    pd = (1 - dp, lax.rem(ep + 2, 4))
    pc = (dp, ep + 1 - 2 * lax.rem(ep, 2))
    e0 = dp * EL

    def a_copy(kind, i, s):
        if kind == 'k':
            return pltpu.make_async_copy(wk, ra.at[s, :, pl.ds(0, QT)], sem_a.at[s])
        if kind == 'v':
            return pltpu.make_async_copy(wv, ra.at[s, :, pl.ds(0, QT)], sem_a.at[s])
        if kind == 'q':
            c = pl.multiple_of(i * QT, QT)
            return pltpu.make_async_copy(wq.at[:, pl.ds(c, QT)], ra.at[s, :, pl.ds(0, QT)], sem_a.at[s])
        if kind in ('w1', 'w3'):
            c = pl.multiple_of(i * FE, FE)
            return pltpu.make_async_copy((w1 if kind == 'w1' else w3).at[:, pl.ds(c, FE)], ra.at[s], sem_a.at[s])
        return pltpu.make_async_copy((ue1 if kind == 'e1' else ue3).at[e0 + i], ra.at[s], sem_a.at[s])

    def a_start(t, lo, hi):
        s = lax.rem(t, NA)

        def pairs(first, last, names, base):
            a, b = max(first, lo), min(last, hi)
            if a >= b:
                return
            for par in (0, 1):
                @pl.when((t >= a) & (t < b) & (lax.rem(t - first, 2) == par))
                def _():
                    a_copy(names[par], base + (t - first) // 2, s).start()

        if lo < A_FF1:
            @pl.when(t < A_FF1)
            def _():
                a_copy('q', t - 2, s).start()
        pairs(A_FF1, A_EXP, ('w1', 'w3'), 0)
        pairs(A_EXP, A_FF2, ('e1', 'e3'), 0)
        pairs(A_FF2, A_END, ('w1', 'w3'), N1)

    def b_copy(kind, i, s):
        if kind == 'wo':
            return pltpu.make_async_copy(
                wo.at[pl.ds(lax.rem(i, 2) * 4, 4), :, pl.ds(pl.multiple_of((i // 2) * CW, CW), CW)],
                rb.at[s, :, pl.ds(0, QT), :], sem_b.at[s])
        if kind == 'w2':
            return pltpu.make_async_copy(
                w2.at[pl.ds(lax.rem(i, 2) * 4, 4), :, pl.ds(pl.multiple_of((i // 2) * CW, CW), CW)],
                rb.at[s], sem_b.at[s])
        return pltpu.make_async_copy(
            ue2.at[pl.ds(e0 + lax.rem(i, 4) * 4, 4), :, pl.ds(pl.multiple_of((i // 4) * CW, CW), CW)],
            rb.at[s], sem_b.at[s])

    def b_start(t, lo, hi):
        s = lax.rem(t, NB)
        for first, last, name in ((0, B_EXP, 'wo'), (B_EXP, B_W2, 'e2'), (B_W2, B_END, 'w2')):
            a, b = max(first, lo), min(last, hi)
            if a >= b:
                continue

            @pl.when((t >= a) & (t < b))
            def _():
                b_copy(name, t - first, s).start()

    specs = {}

    def rdma(key, src, dst, to):
        i = specs.setdefault(key, len(specs))
        return pltpu.make_async_remote_copy(src_ref=src, dst_ref=dst, send_sem=send.at[i], recv_sem=recv.at[i],
                                            device_id=to, device_id_type=MESH)

    ag = {
        'ix': lambda: rdma('ix', info.at[0], info.at[2], px),
        'iy': lambda: rdma('iy', info.at[0], info.at[3], py),
        'id': lambda: rdma('id', info.at[0], info.at[6], pd),
        'ic': lambda: rdma('ic', info.at[0], info.at[1], pc),
        'x0': lambda: rdma('x0', u.at[0, 0], u.at[2, 0], px),
        'x1': lambda: rdma('x1', u.at[0, 1], u.at[2, 1], px),
        'y1': lambda: rdma('y1', u.at[0, 1], u.at[3, 1], py),
        'y0': lambda: rdma('y0', u.at[0, 0], u.at[3, 0], py),
        'c': lambda: rdma('c', u.at[0], u.at[1], pc),
        'd0': lambda: rdma('d0', u.at[2, 0], u.at[6, 0], py),
        'd1': lambda: rdma('d1', u.at[3, 1], u.at[6, 1], px),
        'cx': lambda: rdma('cx', u.at[2], u.at[4], pc),
        'cy': lambda: rdma('cy', u.at[3], u.at[5], pc),
        'cd': lambda: rdma('cd', u.at[6], u.at[7], pc),
        'icx': lambda: rdma('icx', info.at[2], info.at[4], pc),
        'icy': lambda: rdma('icy', info.at[3], info.at[5], pc),
        'icd': lambda: rdma('icd', info.at[6], info.at[7], pc),
    }
    for key in ag:
        specs.setdefault(key, len(specs))

    def rs(name, c):
        key = (name, c)
        if name[0] == 'c':
            n = int(name[1])
            return rdma(key, pp.at[c, 4 + n], rc.at[c, n], pc)
        if name == 'xa':
            return rdma(key, pp.at[c, 1, 0], r1.at[c, 0], px)
        if name == 'xb':
            return rdma(key, pp.at[c, 3, 0], r1.at[c, 1], px)
        if name == 'ya':
            return rdma(key, pp.at[c, 2, 1], r1.at[c, 2], py)
        if name == 'yb':
            return rdma(key, pp.at[c, 3, 1], r1.at[c, 3], py)
        if name == 'y2':
            return rdma(key, pp.at[c, 2, 0], r2.at[c, 0], py)
        return rdma(key, pp.at[c, 1, 1], r2.at[c, 1], px)

    def rs_first(c):
        for q in (3, 1, 2, 0):
            rs('c%d' % q, c).wait_recv()
            pp[c, q] = pp[c, q] + rc[c, q]
            for name in ((), ('xa',), ('ya',), ('xb', 'yb'))[q]:
                rs(name, c).start()

    def rs_second(c):
        rs('xb', c).wait_recv()
        pp[c, 2, 0] = pp[c, 2, 0] + r1[c, 1]
        rs('y2', c).start()
        rs('yb', c).wait_recv()
        pp[c, 1, 1] = pp[c, 1, 1] + r1[c, 3]
        rs('x2', c).start()

    def rs_last(c):
        lo = slice(c * CW, c * CW + HW)
        hi = slice(c * CW + HW, (c + 1) * CW)
        rs('xa', c).wait_recv()
        rs('y2', c).wait_recv()
        out[0, :, lo] = (fs[:, lo] + ((pp[c, 0, 0] + r1[c, 0]) + r2[c, 0])).astype(bf16)
        rs('ya', c).wait_recv()
        rs('x2', c).wait_recv()
        out[0, :, hi] = (fs[:, hi] + ((pp[c, 0, 1] + r1[c, 2]) + r2[c, 1])).astype(bf16)

    barrier = pltpu.get_barrier_semaphore()
    for to in (px, py, pd, pc):
        pl.semaphore_signal(barrier, inc=1, device_id=to, device_id_type=MESH)
    a_copy('k', 0, 0).start()
    a_copy('v', 0, 1).start()
    for i in range(NA - 2):
        a_copy('q', i, 2 + i).start()
    for i in range(NB):
        b_copy('wo', i, i).start()

    def norms(i, _):
        rows = pl.ds(pl.multiple_of(i * 16, 16), 16)
        xf = h0[0, rows, :].astype(f32)
        xr = xf * lax.rsqrt(jnp.mean(xf * xf, axis=-1, keepdims=True) + EPS)
        un = (xr * nm[...].astype(f32)[None, :]).astype(bf16)
        u[0, 0, rows, :] = un[:, :D // 2]
        u[0, 1, rows, :] = un[:, D // 2:]
        xz[rows, :] = (xr * na[...].astype(f32)[None, :]).astype(bf16)
        return 0

    lax.fori_loop(0, T // 16, norms, 0, unroll=4)
    pl.semaphore_wait(barrier, 4)
    for key in ('x0', 'y1', 'c', 'x1', 'y0'):
        ag[key]().start()

    logits = _dot(u[0, 0], wr[pl.ds(0, D // 2), :]) + _dot(u[0, 1], wr[pl.ds(D // 2, D // 2), :])
    lt = logits.T
    idt = idx[0].astype(f32)
    slt = slot[0].astype(f32)
    ex = lax.broadcasted_iota(jnp.int32, (T, T), 0).astype(f32)
    sel = jnp.concatenate(
        [jnp.sum(jnp.where(ex == idt[j:j + 1, :], lt, 0.0), axis=0, keepdims=True) for j in range(TOP)], axis=0)
    gate = jnp.exp(sel - jnp.max(sel, axis=0, keepdims=True))
    gate = gate / jnp.sum(gate, axis=0, keepdims=True)
    info[0, pl.ds(0, TOP), :] = idt * float(CAP) + slt
    info[0, pl.ds(TOP, TOP), :] = gate

    cs, sn = cos[...], sin[...]

    def rope(v):
        return (v * cs + pltpu.roll(v, HEAD // 2, 1) * sn).astype(bf16)

    a_copy('k', 0, 0).wait()
    kf = _dot(xz[...], ra[0, :, pl.ds(0, QT)])
    a_copy('q', 2, 0).start()
    for n in range(4):
        kk[n] = rope(kf[:, n * HEAD:(n + 1) * HEAD])
    for key in ('ix', 'iy', 'id', 'ic'):
        ag[key]().start()
    a_copy('v', 0, 1).wait()
    vf = _dot(xz[...], ra[1, :, pl.ds(0, QT)])
    a_copy('q', 3, 1).start()
    for n in range(4):
        vv[n] = vf[:, n * HEAD:(n + 1) * HEAD].astype(bf16)
    causal = lax.broadcasted_iota(jnp.int32, (T, T), 0) >= lax.broadcasted_iota(jnp.int32, (T, T), 1)

    def q_dot(i, dst):
        s = lax.rem(2 + i, NA)
        a_copy('q', i, s).wait()
        dst[...] = _dot(xz[...], ra[s, :, pl.ds(0, QT)])
        a_start(2 + i + NA, 2 + NA, A_FF1 + NA)

    def q_heads(i, src):
        kg, vg = kk[i // 2], vv[i // 2]
        qs = jnp.concatenate([rope(src[:, n * HEAD:(n + 1) * HEAD]) for n in range(4)], axis=0)
        sc = lax.dot_general(qs, kg, (((1,), (1,)), ((), ())), preferred_element_type=f32) * HEAD ** -0.5
        ps = []
        for n in range(4):
            sm = jnp.where(causal, sc[n * T:(n + 1) * T], -jnp.inf)
            p = jnp.exp(sm - jnp.max(sm, axis=-1, keepdims=True))
            ps.append((p * (1.0 / jnp.sum(p, axis=-1, keepdims=True))).astype(bf16))
        o = _dot(jnp.concatenate(ps, axis=0), vg)
        for n in range(4):
            g[i, :, n * HEAD:(n + 1) * HEAD] = o[n * T:(n + 1) * T].astype(bf16)

    def q_pair(k, _):
        q_dot(2 * k + 1, qb)
        q_heads(2 * k, qa)

        @pl.when(k == Q_FWD)
        def _():
            ag['x0']().wait_recv()
            ag['d0']().start()
            ag['y1']().wait_recv()
            ag['d1']().start()

        q_dot(2 * k + 2, qa)
        q_heads(2 * k + 1, qb)
        return 0

    q_dot(0, qa)
    lax.fori_loop(0, NQ // 2 - 1, q_pair, 0)
    q_dot(NQ - 1, qb)
    q_heads(NQ - 2, qa)
    q_heads(NQ - 1, qb)

    def wo_step(n, _):
        cols = pl.ds(pl.multiple_of(n * CW, CW), CW)
        acc = h0[0, :, cols].astype(f32)
        prod = None
        for half in range(2):
            t = 2 * n + half
            s = lax.rem(t, NB)
            b_copy('wo', t, s).wait()
            for i in range(4):
                term = _dot(g[half * 4 + i, :, pl.ds(0, QT)], rb[s, i, pl.ds(0, QT), :])
                prod = term if prod is None else prod + term
            b_start(t + NB, NB, B_EXP + NB)
        ar[:, cols] = (acc + prod).astype(bf16)
        return 0

    lax.fori_loop(0, D // CW, wo_step, 0)

    def znorm(i, _):
        rows = pl.ds(pl.multiple_of(i * 16, 16), 16)
        xf = ar[rows, :].astype(f32)
        xr = xf * lax.rsqrt(jnp.mean(xf * xf, axis=-1, keepdims=True) + EPS)
        xz[rows, :] = (xr * nf[...].astype(f32)[None, :]).astype(bf16)
        return 0

    lax.fori_loop(0, T // 16, znorm, 0, unroll=4)

    for key in ('ix', 'iy', 'id', 'x1', 'y0'):
        ag[key]().wait_recv()
    for key in ('icx', 'icy', 'icd', 'cx', 'cy'):
        ag[key]().start()

    def gated(lhs, t, kinds, i, hi):
        s1, s3 = lax.rem(t, NA), lax.rem(t + 1, NA)
        a_copy(kinds[0], i, s1).wait()
        h1 = _dot(lhs, ra[s1])
        a_copy(kinds[1], i, s3).wait()
        h3 = _dot(lhs, ra[s3])
        for k in (0, 1):
            a_start(t + NA + k, *hi)
        return (h1 * jax.nn.sigmoid(h1) * h3).astype(bf16)

    def ffn1(i, _):
        g[i] = gated(xz[...], A_FF1 + 2 * i, ('w1', 'w3'), i, (A_FF1 + NA, A_EXP + NA))
        return 0

    lax.fori_loop(0, N1, ffn1, 0)

    base = ((ep * 32 + e0) * CAP).astype(f32)

    def build(r, _):
        for half in range(2):
            row = lax.broadcasted_iota(jnp.int32, (T, T), 0).astype(f32) + (base + float(half * T))
            w = jnp.zeros((T, T), f32)
            d = jnp.zeros((T, T), f32)
            for j in range(TOP):
                hit = row == info[r, pl.ds(j, 1), :]
                w = jnp.where(hit, info[r, pl.ds(TOP + j, 1), :], w)
                d = jnp.where(hit, 1.0, d)
            wt = w.T
            hi = wt.astype(bf16)
            rest = wt - hi.astype(f32)
            mid = rest.astype(bf16)
            low = (rest - mid.astype(f32)).astype(bf16)
            for n, part in enumerate((hi, mid, low)):
                ws[r, pl.ds(n * T, T), half * T:(half + 1) * T] = part
            db = d.astype(bf16)
            for c in range(4):
                rows = _dot(db, u[r, c // 2, :, (c % 2) * 512:(c % 2 + 1) * 512]).astype(bf16)
                x[pl.ds(half * 8, 8), pl.ds(pl.multiple_of(r * CAP, CAP), CAP), c * 512:(c + 1) * 512] = (
                    rows.reshape(8, CAP, 512))
        return 0

    for key in ('ic', 'icx', 'icy', 'c', 'cx', 'cy'):
        ag[key]().wait_recv()
    lax.fori_loop(0, 6, build, 0)
    for key in ('d0', 'd1'):
        ag[key]().wait_recv()
    ag['cd']().start()
    build(6, 0)
    for key in ('icd', 'cd'):
        ag[key]().wait_recv()
    build(7, 0)

    def experts(e, _):
        x[e, :, :FE] = gated(x[e], A_EXP + 2 * e, ('e1', 'e3'), e, (A_EXP + NA, A_FF2 + NA))
        return 0

    lax.fori_loop(0, EL, experts, 0)

    YC = 1024

    def chunk(c):
        def part(k, _):
            t = B_EXP + 4 * c + k
            s = lax.rem(t, NB)
            b_copy('e2', 4 * c + k, s).wait()
            for i in range(4):
                x[4 * k + i, :, YC:YC + CW] = _dot(x[4 * k + i, :, :FE], rb[s, i]).astype(bf16)
            b_start(t + NB, B_EXP + NB, B_W2 + NB)
            return 0

        if c == 0:
            lax.fori_loop(0, 4, part, 0)
        else:
            lax.fori_loop(0, 2, part, 0)
            rs_first(c - 1)
            lax.fori_loop(2, 4, part, 0)

        for q in (7, 5, 6, 4, 3, 1, 2, 0):
            r = PLACE[q]
            yr = x[:, r * CAP:(r + 1) * CAP, YC:YC + CW].reshape(2 * T, CW)
            three = _dot(ws[r], yr)
            m = (three[:T] + three[T:2 * T]) + three[2 * T:]
            pp[c, q, 0] = m[:, :HW]
            pp[c, q, 1] = m[:, HW:]
            if q >= 4:
                rs('c%d' % (q - 4), c).start()

    for c in range(NC):
        chunk(c)

    def ffn2(i, _):
        g[i] = gated(xz[...], A_FF2 - 2 * N1 + 2 * i, ('w1', 'w3'), i, (A_FF2 + NA, A_END))
        for at, fn in ((N1, lambda: rs_first(NC - 1)), (N1 + 1, lambda: rs_second(0)), (N1 + 3, lambda: rs_second(1)),
                       (NF - 1, lambda: rs_second(2))):
            @pl.when(i == at)
            def _():
                fn()
        return 0

    lax.fori_loop(N1, NF, ffn2, 0)

    def w2_step(n, _):
        cols = pl.ds(pl.multiple_of(n * CW, CW), CW)
        prod = None
        for half in range(2):
            t = B_W2 + 2 * n + half
            s = lax.rem(t, NB)
            b_copy('w2', 2 * n + half, s).wait()
            for i in range(4):
                term = _dot(g[half * 4 + i], rb[s, i])
                prod = term if prod is None else prod + term
            b_start(t + NB, B_W2 + NB, B_END)
        fs[:, cols] = ar[:, cols].astype(f32) + prod
        return 0

    lax.fori_loop(0, 4, w2_step, 0)
    rs_second(3)
    for c in range(NC):
        rs_last(c)
    for key in ag:
        ag[key]().wait_send()
    for c in range(NC):
        for name in ('c0', 'c1', 'c2', 'c3', 'xa', 'xb', 'ya', 'yb', 'y2', 'x2'):
            rs(name, c).wait_send()


def solution(mesh):
    ang = (np.arange(T, dtype=np.float32)[:, None]
           * (ROPE_BASE ** (-2.0 * np.arange(HEAD // 2) / HEAD)).astype(np.float32)[None, :])
    cos = np.cos(ang.astype(np.float64)).astype(np.float32)
    sin = np.sin(ang.astype(np.float64)).astype(np.float32)
    cos2 = np.concatenate([cos, cos], axis=1)
    sin2 = np.concatenate([-sin, sin], axis=1)
    ncopies = 17 + 10 * NC

    def local(h0, idx, slot, na, wq, wk, wv, wo, nf, w1, w3, w2, nm, wr, ue1, ue3, ue2):
        vm = pl.BlockSpec(memory_space=pltpu.VMEM)
        hb = pl.BlockSpec(memory_space=pl.ANY)
        return pl.pallas_call(
            _kernel,
            out_shape=jax.ShapeDtypeStruct(h0.shape, bf16),
            in_specs=[vm] * 9 + [hb] * 10,
            out_specs=vm,
            scratch_shapes=[
                pltpu.VMEM((T, D), bf16),
                pltpu.VMEM((T, D), bf16),
                pltpu.VMEM((T, D), f32),
                pltpu.VMEM((T, QT), f32),
                pltpu.VMEM((T, QT), f32),
                pltpu.VMEM((8, 2, T, D // 2), bf16),
                pltpu.VMEM((8, 2 * TOP, T), f32),
                pltpu.VMEM((8, 3 * T, 2 * T), bf16),
                pltpu.VMEM((EL, T, D), bf16),
                pltpu.VMEM((4, T, HEAD), bf16),
                pltpu.VMEM((4, T, HEAD), bf16),
                pltpu.VMEM((NF, T, FE), bf16),
                pltpu.VMEM((NC, 8, 2, T, HW), f32),
                pltpu.VMEM((NC, 4, 2, T, HW), f32),
                pltpu.VMEM((NC, 4, T, HW), f32),
                pltpu.VMEM((NC, 2, T, HW), f32),
                pltpu.VMEM((NA, D, FE), bf16),
                pltpu.VMEM((NB, 4, FE, CW), bf16),
                pltpu.SemaphoreType.DMA((NA,)),
                pltpu.SemaphoreType.DMA((NB,)),
                pltpu.SemaphoreType.DMA((ncopies,)),
                pltpu.SemaphoreType.DMA((ncopies,)),
            ],
            compiler_params=pltpu.CompilerParams(collective_id=0, has_side_effects=True,
                                                 vmem_limit_bytes=67043328),
            name='scmoe',
        )(h0, jnp.swapaxes(idx, 1, 2), jnp.swapaxes(slot, 1, 2), na, nf, nm,
          jnp.asarray(cos2), jnp.asarray(sin2), wr, wq, wk, wv, wo.reshape(8, QT, D),
          w1, w3, w2.reshape(8, FE, D), ue1, ue3, ue2)

    rows = P(('dp', 'ep'))
    in_specs = (rows,) * 3 + (P(),) * 11 + (P('ep'),) * 3
    return jax.shard_map(local, mesh=mesh, in_specs=in_specs, out_specs=rows, check_vma=False)
```

```python
import functools

import jax
import jax.numpy as jnp
import numpy as np
from jax import lax
from jax.experimental import pallas as pl
from jax.experimental.pallas import tpu as pltpu
from jax.sharding import PartitionSpec as P

MESH = pl.DeviceIdType.MESH
HEAD = 128
EPS = 1e-6
ROPE_BASE = 10000.0

T, D, FE, FF, TOP, CAP = 128, 2048, 768, 6144, 8, 16
EL = 16
QT = 512
CW = 512
NC = D // CW
HW = CW // 2
NA = 4
NB = 4
NQ = 8
Q_FWD = 1
E_FWD = (0, 2, 5)
PLACE = (0, 2, 3, 6, 1, 4, 5, 7)
NF = FF // FE
KH = D // 2
A_EXP = 2 + NQ
A_FFN = A_EXP + 2 * EL
A_END = A_FFN + 2 * NF
B_WO = 4 * NC
B_W2 = B_WO + 8
B_END = B_W2 + 8
RC = 16 * NC
R1 = RC + 8 * NC
R2 = R1 + 4 * NC
NBLK = R2 + 2 * NC

f32, bf16 = jnp.float32, jnp.bfloat16


def _dot(a, b):
    return jnp.dot(a, b, preferred_element_type=f32)


def _mult(v):
    return v if isinstance(v, int) else pl.multiple_of(v, CW)


def _kernel(h0, idx, slot, na, nf, nm, cos, sin, wr, wq, wk, wv, wo, w1, w3, w2, ue1, ue3, ue2, out,
            xz, ar, qa, qb, u, info, ws, ds, x, kk, vv, g, big, ra, rb,
            sem_a, sem_b, send, recv, ready):
    dp, ep = lax.axis_index('dp'), lax.axis_index('ep')
    px = (dp, lax.rem(ep + 2, 4))
    py = (1 - dp, ep)
    pd = (1 - dp, lax.rem(ep + 2, 4))
    pc = (dp, ep + 1 - 2 * lax.rem(ep, 2))
    e0 = dp * EL

    def a_copy(kind, i, s):
        if kind == 'k':
            return pltpu.make_async_copy(wk, ra.at[s, :, pl.ds(0, QT)], sem_a.at[s])
        if kind == 'v':
            return pltpu.make_async_copy(wv, ra.at[s, :, pl.ds(0, QT)], sem_a.at[s])
        if kind == 'q':
            c = pl.multiple_of(i * QT, QT)
            return pltpu.make_async_copy(wq.at[:, pl.ds(c, QT)], ra.at[s, :, pl.ds(0, QT)], sem_a.at[s])
        if kind in ('w1', 'w3'):
            c = pl.multiple_of(i * FE, FE)
            return pltpu.make_async_copy((w1 if kind == 'w1' else w3).at[:, pl.ds(c, FE)], ra.at[s], sem_a.at[s])
        raise ValueError(kind)

    def e_start(t, s):
        k = t - A_EXP
        first = k < EL
        e = e0 + jnp.where(first, k, 2 * EL - 1 - k)
        rows = pl.ds(pl.multiple_of(jnp.where(first, 0, KH), KH), KH)
        pltpu.make_async_copy(ue1.at[e, rows, :], ra.at[s, pl.ds(0, KH), :], sem_a.at[s]).start()
        pltpu.make_async_copy(ue3.at[e, rows, :], ra.at[s, pl.ds(KH, KH), :], sem_a.at[s]).start()

    def e_wait(s):
        pltpu.make_async_copy(ue1.at[e0], ra.at[s], sem_a.at[s]).wait()

    def a_start(t, lo, hi):
        s = lax.rem(t, NA)
        if lo < A_EXP:
            @pl.when(t < A_EXP)
            def _():
                a_copy('q', t - 2, s).start()
        if lo < A_FFN and hi > A_EXP:
            @pl.when((t >= A_EXP) & (t < A_FFN))
            def _():
                e_start(t, s)
        if hi > A_FFN:
            for par in (0, 1):
                @pl.when((t >= A_FFN) & (t < A_END) & (lax.rem(t - A_FFN, 2) == par))
                def _():
                    a_copy(('w1', 'w3')[par], (t - A_FFN) // 2, s).start()

    def b_copy(kind, i, s):
        if kind == 'wo':
            return pltpu.make_async_copy(
                wo.at[pl.ds(i % 2 * 4, 4), :, pl.ds(_mult(i // 2 * CW), CW)],
                rb.at[s, :, pl.ds(0, QT), :], sem_b.at[s])
        if kind == 'w2':
            return pltpu.make_async_copy(
                w2.at[pl.ds(i % 2 * 4, 4), :, pl.ds(_mult(i // 2 * CW), CW)],
                rb.at[s], sem_b.at[s])
        return pltpu.make_async_copy(
            ue2.at[pl.ds(e0 + i % 4 * 4, 4), :, pl.ds(_mult(i // 4 * CW), CW)],
            rb.at[s], sem_b.at[s])

    def b_start(t, lo, hi):
        s = lax.rem(t, NB)
        for first, last, name in ((0, B_WO, 'e2'), (B_WO, B_W2, 'wo'), (B_W2, B_END, 'w2')):
            a, b = max(first, lo), min(last, hi)
            if a >= b:
                continue

            @pl.when((t >= a) & (t < b))
            def _():
                b_copy(name, t - first, s).start()

    specs = {}

    def rdma(key, src, dst, to):
        i = specs.setdefault(key, len(specs))
        return pltpu.make_async_remote_copy(src_ref=src, dst_ref=dst, send_sem=send.at[i], recv_sem=recv.at[i],
                                            device_id=to, device_id_type=MESH)

    ag = {
        'ix': lambda: rdma('ix', info.at[0], info.at[2], px),
        'iy': lambda: rdma('iy', info.at[0], info.at[3], py),
        'id': lambda: rdma('id', info.at[0], info.at[6], pd),
        'ic': lambda: rdma('ic', info.at[0], info.at[1], pc),
        'c0': lambda: rdma('c0', u.at[0, pl.ds(0, 2)], u.at[1, pl.ds(0, 2)], pc),
        'c1': lambda: rdma('c1', u.at[0, pl.ds(2, 2)], u.at[1, pl.ds(2, 2)], pc),
        'x0': lambda: rdma('x0', u.at[0, 0], u.at[2, 0], px),
        'y0': lambda: rdma('y0', u.at[0, 0], u.at[3, 0], py),
        'x1': lambda: rdma('x1', u.at[0, 1], u.at[2, 1], px),
        'y1': lambda: rdma('y1', u.at[0, 1], u.at[3, 1], py),
        'x2': lambda: rdma('x2', u.at[0, 2], u.at[2, 2], px),
        'y2': lambda: rdma('y2', u.at[0, 2], u.at[3, 2], py),
        'x3': lambda: rdma('x3', u.at[0, 3], u.at[2, 3], px),
        'y3': lambda: rdma('y3', u.at[0, 3], u.at[3, 3], py),
        'd0': lambda: rdma('d0', u.at[2, 0], u.at[6, 0], py),
        'd1': lambda: rdma('d1', u.at[3, 1], u.at[6, 1], px),
        'd2': lambda: rdma('d2', u.at[2, 2], u.at[6, 2], py),
        'd3': lambda: rdma('d3', u.at[3, 3], u.at[6, 3], px),
        'cx0': lambda: rdma('cx0', u.at[2, pl.ds(0, 2)], u.at[4, pl.ds(0, 2)], pc),
        'cx1': lambda: rdma('cx1', u.at[2, pl.ds(2, 2)], u.at[4, pl.ds(2, 2)], pc),
        'cy0': lambda: rdma('cy0', u.at[3, pl.ds(0, 2)], u.at[5, pl.ds(0, 2)], pc),
        'cy1': lambda: rdma('cy1', u.at[3, pl.ds(2, 2)], u.at[5, pl.ds(2, 2)], pc),
        'cd0': lambda: rdma('cd0', u.at[6, pl.ds(0, 2)], u.at[7, pl.ds(0, 2)], pc),
        'cd1': lambda: rdma('cd1', u.at[6, pl.ds(2, 2)], u.at[7, pl.ds(2, 2)], pc),
        'icx': lambda: rdma('icx', info.at[2], info.at[4], pc),
        'icy': lambda: rdma('icy', info.at[3], info.at[5], pc),
        'icd': lambda: rdma('icd', info.at[6], info.at[7], pc),
    }
    for key in ag:
        specs.setdefault(key, len(specs))

    def sums(c, q, half=0):
        return c * 16 + q * 2 + half

    def rs(name, c):
        key = (name, c)
        if name[0] == 'c':
            n = int(name[1])
            return rdma(key, big.at[pl.ds(sums(c, 4 + n), 2)], big.at[pl.ds(RC + c * 8 + n * 2, 2)], pc)
        src, dst, to = {
            'xa': (sums(c, 1, 0), R1 + c * 4, px),
            'xb': (sums(c, 3, 0), R1 + c * 4 + 1, px),
            'ya': (sums(c, 2, 1), R1 + c * 4 + 2, py),
            'yb': (sums(c, 3, 1), R1 + c * 4 + 3, py),
            'y2': (sums(c, 2, 0), R2 + c * 2, py),
            'x2': (sums(c, 1, 1), R2 + c * 2 + 1, px),
        }[name]
        return rdma(key, big.at[src], big.at[dst], to)

    def rs_first(c):
        for q in (3, 1, 2, 0):
            rs('c%d' % q, c).wait_recv()
            for half in range(2):
                k = sums(c, q, half)
                big[k] = big[k] + big[RC + c * 8 + q * 2 + half]
            for name in ((), ('xa',), ('ya',), ('xb', 'yb'))[q]:
                rs(name, c).start()

    def rs_second(c):
        rs('xb', c).wait_recv()
        big[sums(c, 2, 0)] = big[sums(c, 2, 0)] + big[R1 + c * 4 + 1]
        rs('y2', c).start()
        rs('yb', c).wait_recv()
        big[sums(c, 1, 1)] = big[sums(c, 1, 1)] + big[R1 + c * 4 + 3]
        rs('x2', c).start()

    def rs_last(c, f):
        rs('xa', c).wait_recv()
        rs('y2', c).wait_recv()
        m = (big[sums(c, 0, 0)] + big[R1 + c * 4]) + big[R2 + c * 2]
        out[0, :, c * CW:c * CW + HW] = (f[:, :HW] + m).astype(bf16)
        rs('ya', c).wait_recv()
        rs('x2', c).wait_recv()
        m = (big[sums(c, 0, 1)] + big[R1 + c * 4 + 2]) + big[R2 + c * 2 + 1]
        out[0, :, c * CW + HW:(c + 1) * CW] = (f[:, HW:] + m).astype(bf16)

    barrier = pltpu.get_barrier_semaphore()
    for to in (px, py, pd, pc):
        pl.semaphore_signal(barrier, inc=1, device_id=to, device_id_type=MESH)
    a_copy('k', 0, 0).start()
    a_copy('v', 0, 1).start()
    for i in range(NA - 2):
        a_copy('q', i, 2 + i).start()

    def norms(i, _):
        rows = pl.ds(pl.multiple_of(i * 16, 16), 16)
        xf = h0[0, rows, :].astype(f32)
        xr = xf * lax.rsqrt(jnp.mean(xf * xf, axis=-1, keepdims=True) + EPS)
        un = (xr * nm[...].astype(f32)[None, :]).astype(bf16)
        for k in range(4):
            u[0, k, rows, :] = un[:, k * 512:(k + 1) * 512]
        xz[rows, :] = (xr * na[...].astype(f32)[None, :]).astype(bf16)
        return 0

    lax.fori_loop(0, T // 16, norms, 0, unroll=4)
    pl.semaphore_wait(barrier, 4)
    for key in ('x0', 'y1', 'c0', 'x1', 'y0', 'c1'):
        ag[key]().start()

    logits = _dot(u[0, 0], wr[pl.ds(0, 512), :])
    for k in range(1, 4):
        logits = logits + _dot(u[0, k], wr[pl.ds(k * 512, 512), :])
    lt = logits.T
    idt = idx[0].astype(f32)
    slt = slot[0].astype(f32)
    ex = lax.broadcasted_iota(jnp.int32, (T, T), 0).astype(f32)
    sel = jnp.concatenate(
        [jnp.sum(jnp.where(ex == idt[j:j + 1, :], lt, 0.0), axis=0, keepdims=True) for j in range(TOP)], axis=0)
    gate = jnp.exp(sel - jnp.max(sel, axis=0, keepdims=True))
    gate = gate / jnp.sum(gate, axis=0, keepdims=True)
    info[0, pl.ds(0, TOP), :] = idt * float(CAP) + slt
    info[0, pl.ds(TOP, TOP), :] = gate

    cs, sn = cos[...], sin[...]

    def rope(v):
        return (v * cs + pltpu.roll(v, HEAD // 2, 1) * sn).astype(bf16)

    a_copy('k', 0, 0).wait()
    kf = _dot(xz[...], ra[0, :, pl.ds(0, QT)])
    a_copy('q', 2, 0).start()
    for n in range(4):
        kk[n] = rope(kf[:, n * HEAD:(n + 1) * HEAD])
    for key in ('ix', 'iy', 'id', 'ic'):
        ag[key]().start()
    a_copy('v', 0, 1).wait()
    vf = _dot(xz[...], ra[1, :, pl.ds(0, QT)])
    a_copy('q', 3, 1).start()
    for n in range(4):
        vv[n] = vf[:, n * HEAD:(n + 1) * HEAD].astype(bf16)
    causal = lax.broadcasted_iota(jnp.int32, (T, T), 0) >= lax.broadcasted_iota(jnp.int32, (T, T), 1)

    def q_dot(i, dst):
        s = lax.rem(2 + i, NA)
        a_copy('q', i, s).wait()
        dst[...] = _dot(xz[...], ra[s, :, pl.ds(0, QT)])
        a_start(2 + i + NA, 2 + NA, A_EXP + NA)

    def q_heads(i, src):
        kg, vg = kk[i // 2], vv[i // 2]
        qs = jnp.concatenate([rope(src[:, n * HEAD:(n + 1) * HEAD]) for n in range(4)], axis=0)
        sc = lax.dot_general(qs, kg, (((1,), (1,)), ((), ())), preferred_element_type=f32) * HEAD ** -0.5
        ps = []
        for n in range(4):
            sm = jnp.where(causal, sc[n * T:(n + 1) * T], -jnp.inf)
            p = jnp.exp(sm - jnp.max(sm, axis=-1, keepdims=True))
            ps.append((p * (1.0 / jnp.sum(p, axis=-1, keepdims=True))).astype(bf16))
        o = _dot(jnp.concatenate(ps, axis=0), vg)
        for n in range(4):
            g[i, :, n * HEAD:(n + 1) * HEAD] = o[n * T:(n + 1) * T].astype(bf16)

    def q_pair(k, _):
        q_dot(2 * k + 1, qb)
        q_heads(2 * k, qa)

        @pl.when(k == Q_FWD)
        def _():
            ag['x0']().wait_recv()
            ag['d0']().start()
            ag['y1']().wait_recv()
            ag['d1']().start()
            for key in ('x2', 'y3', 'x3', 'y2'):
                ag[key]().start()

        q_dot(2 * k + 2, qa)
        q_heads(2 * k + 1, qb)
        b_copy('e2', k, k).start()
        return 0

    q_dot(0, qa)
    lax.fori_loop(0, NQ // 2 - 1, q_pair, 0)
    q_dot(NQ - 1, qb)
    b_copy('e2', 3, 3).start()
    for key in ('ix', 'iy', 'id', 'x1', 'y0'):
        ag[key]().wait_recv()
    for key in ('icx', 'icy', 'icd', 'cx0', 'cy0'):
        ag[key]().start()
    q_heads(NQ - 2, qa)
    q_heads(NQ - 1, qb)

    base = ((ep * 32 + e0) * CAP).astype(f32)

    def weights(r):
        for half in range(2):
            row = lax.broadcasted_iota(jnp.int32, (T, T), 0).astype(f32) + (base + float(half * T))
            w = jnp.zeros((T, T), f32)
            d = jnp.zeros((T, T), f32)
            for j in range(TOP):
                hit = row == info[r, pl.ds(j, 1), :]
                w = jnp.where(hit, info[r, pl.ds(TOP + j, 1), :], w)
                d = jnp.where(hit, 1.0, d)
            wt = w.T
            hi = wt.astype(bf16)
            rest = wt - hi.astype(f32)
            mid = rest.astype(bf16)
            low = (rest - mid.astype(f32)).astype(bf16)
            for n, part in enumerate((hi, mid, low)):
                ws[r, pl.ds(n * T, T), half * T:(half + 1) * T] = part
            ds[r, pl.ds(half * T, T), :] = d.astype(bf16)

    def rows_of(r, k):
        rows = _dot(ds[r], u[r, k]).astype(bf16)
        x[:, pl.ds(pl.multiple_of(r * CAP, CAP), CAP), k * 512:(k + 1) * 512] = rows.reshape(EL, CAP, 512)

    def build(r, _):
        weights(r)
        for k in range(2):
            rows_of(r, k)
        return 0

    for key in ('ic', 'c0'):
        ag[key]().wait_recv()
    lax.fori_loop(0, 4, build, 0)
    for key in ('d0', 'd1'):
        ag[key]().wait_recv()
    ag['cd0']().start()
    for key in ('icx', 'icy', 'icd', 'cx0', 'cy0'):
        ag[key]().wait_recv()
    lax.fori_loop(4, 7, build, 0)
    ag['cd0']().wait_recv()
    build(7, 0)

    def first_half(e, _):
        s = lax.rem(A_EXP + e, NA)
        e_wait(s)
        for n in range(2):
            h = _dot(x[e, :, :KH], ra[s, pl.ds(n * KH, KH), :])
            for j in range(3):
                big[e * 6 + n * 3 + j] = h[:, j * HW:(j + 1) * HW]
        a_start(A_EXP + e + NA, A_EXP + NA, A_FFN)

        @pl.when(e == E_FWD[0])
        def _():
            ag['x2']().wait_recv()
            ag['d2']().start()
            ag['y3']().wait_recv()
            ag['d3']().start()

        @pl.when(e == E_FWD[1])
        def _():
            for key in ('x3', 'y2'):
                ag[key]().wait_recv()
            for key in ('cx1', 'cy1'):
                ag[key]().start()

        @pl.when(e == E_FWD[2])
        def _():
            for key in ('d2', 'd3'):
                ag[key]().wait_recv()
            ag['cd1']().start()

        @pl.when(e == EL - 9)
        def _():
            for key in ('c1', 'cx1', 'cy1', 'cd1'):
                ag[key]().wait_recv()

        @pl.when(e >= EL - 8)
        def _():
            for k in range(2, 4):
                rows_of(e - (EL - 8), k)
        return 0

    lax.fori_loop(0, EL, first_half, 0)

    def second_half(i, _):
        e = EL - 1 - i
        s = lax.rem(A_EXP + EL + i, NA)
        e_wait(s)
        hs = []
        for n in range(2):
            h = _dot(x[e, :, KH:], ra[s, pl.ds(n * KH, KH), :])
            hs.append([h[:, j * HW:(j + 1) * HW] + big[e * 6 + n * 3 + j] for j in range(3)])
        a_start(A_EXP + EL + i + NA, A_EXP + EL + NA, A_FFN + NA)
        for j in range(3):
            x[e, :, j * HW:(j + 1) * HW] = (hs[0][j] * jax.nn.sigmoid(hs[0][j]) * hs[1][j]).astype(bf16)
        return 0

    lax.fori_loop(0, EL, second_half, 0)
    pl.semaphore_signal(ready, inc=1, device_id=pc, device_id_type=MESH)

    YC = 1024

    def chunk(c):
        def part(k, _):
            t = 4 * c + k
            s = lax.rem(t, NB)
            b_copy('e2', t, s).wait()
            for i in range(4):
                x[4 * k + i, :, YC:YC + CW] = _dot(x[4 * k + i, :, :FE], rb[s, i]).astype(bf16)
            b_start(t + NB, NB, B_WO + NB)
            return 0

        if c == 0:
            lax.fori_loop(0, 4, part, 0)
            pl.semaphore_wait(ready, 1)
        else:
            lax.fori_loop(0, 2, part, 0)
            rs_first(c - 1)
            if c == 2:
                rs_second(0)
            lax.fori_loop(2, 4, part, 0)

        for q in (7, 5, 6, 4, 3, 1, 2, 0):
            r = PLACE[q]
            yr = x[:, r * CAP:(r + 1) * CAP, YC:YC + CW].reshape(2 * T, CW)
            three = _dot(ws[r], yr)
            m = (three[:T] + three[T:2 * T]) + three[2 * T:]
            big[sums(c, q, 0)] = m[:, :HW]
            big[sums(c, q, 1)] = m[:, HW:]
            if q >= 4:
                rs('c%d' % (q - 4), c).start()

    for c in range(NC):
        chunk(c)

    def wo_step(n, _):
        cols = pl.ds(pl.multiple_of(n * CW, CW), CW)
        prod = None
        for half in range(2):
            t = B_WO + 2 * n + half
            s = lax.rem(t, NB)
            b_copy('wo', 2 * n + half, s).wait()
            for i in range(4):
                term = _dot(g[half * 4 + i, :, pl.ds(0, QT)], rb[s, i, pl.ds(0, QT), :])
                prod = term if prod is None else prod + term
            b_start(t + NB, B_WO + NB, B_W2 + NB)
        ar[:, cols] = (h0[0, :, cols].astype(f32) + prod).astype(bf16)

        @pl.when(n == 0)
        def _():
            rs_first(NC - 1)
            rs_second(1)
        return 0

    lax.fori_loop(0, D // CW, wo_step, 0)

    def znorm(i, _):
        rows = pl.ds(pl.multiple_of(i * 16, 16), 16)
        xf = ar[rows, :].astype(f32)
        xr = xf * lax.rsqrt(jnp.mean(xf * xf, axis=-1, keepdims=True) + EPS)
        xz[rows, :] = (xr * nf[...].astype(f32)[None, :]).astype(bf16)
        return 0

    lax.fori_loop(0, T // 16, znorm, 0, unroll=4)

    def ffn(i, _):
        t = A_FFN + 2 * i
        s1, s3 = lax.rem(t, NA), lax.rem(t + 1, NA)
        a_copy('w1', i, s1).wait()
        h1 = _dot(xz[...], ra[s1])
        a_copy('w3', i, s3).wait()
        h3 = _dot(xz[...], ra[s3])
        for k in (0, 1):
            a_start(t + NA + k, A_FFN + NA, A_END)
        g[i] = (h1 * jax.nn.sigmoid(h1) * h3).astype(bf16)
        for at, c in ((1, 2), (5, 3)):
            @pl.when(i == at)
            def _():
                rs_second(c)
        return 0

    lax.fori_loop(0, NF, ffn, 0)

    for n in range(D // CW):
        cols = slice(n * CW, (n + 1) * CW)
        prod = None
        for half in range(2):
            t = B_W2 + 2 * n + half
            s = t % NB
            b_copy('w2', 2 * n + half, s).wait()
            for i in range(4):
                term = _dot(g[half * 4 + i], rb[s, i])
                prod = term if prod is None else prod + term
            if t + NB < B_END:
                b_copy('w2', 2 * n + half + NB, s).start()
        rs_last(n, ar[:, cols].astype(f32) + prod)

    for key in ag:
        ag[key]().wait_send()
    for c in range(NC):
        for name in ('c0', 'c1', 'c2', 'c3', 'xa', 'xb', 'ya', 'yb', 'y2', 'x2'):
            rs(name, c).wait_send()


def solution(mesh):
    ang = (np.arange(T, dtype=np.float32)[:, None]
           * (ROPE_BASE ** (-2.0 * np.arange(HEAD // 2) / HEAD)).astype(np.float32)[None, :])
    cos = np.cos(ang.astype(np.float64)).astype(np.float32)
    sin = np.sin(ang.astype(np.float64)).astype(np.float32)
    cos2 = np.concatenate([cos, cos], axis=1)
    sin2 = np.concatenate([-sin, sin], axis=1)
    ncopies = 27 + 10 * NC

    def local(h0, idx, slot, na, wq, wk, wv, wo, nf, w1, w3, w2, nm, wr, ue1, ue3, ue2):
        vm = pl.BlockSpec(memory_space=pltpu.VMEM)
        hb = pl.BlockSpec(memory_space=pl.ANY)
        return pl.pallas_call(
            _kernel,
            out_shape=jax.ShapeDtypeStruct(h0.shape, bf16),
            in_specs=[vm] * 9 + [hb] * 10,
            out_specs=vm,
            scratch_shapes=[
                pltpu.VMEM((T, D), bf16),
                pltpu.VMEM((T, D), bf16),
                pltpu.VMEM((T, QT), f32),
                pltpu.VMEM((T, QT), f32),
                pltpu.VMEM((8, 4, T, D // 4), bf16),
                pltpu.VMEM((8, 2 * TOP, T), f32),
                pltpu.VMEM((8, 3 * T, 2 * T), bf16),
                pltpu.VMEM((8, 2 * T, T), bf16),
                pltpu.VMEM((EL, T, D), bf16),
                pltpu.VMEM((4, T, HEAD), bf16),
                pltpu.VMEM((4, T, HEAD), bf16),
                pltpu.VMEM((NF, T, FE), bf16),
                pltpu.VMEM((NBLK, T, HW), f32),
                pltpu.VMEM((NA, D, FE), bf16),
                pltpu.VMEM((NB, 4, FE, CW), bf16),
                pltpu.SemaphoreType.DMA((NA,)),
                pltpu.SemaphoreType.DMA((NB,)),
                pltpu.SemaphoreType.DMA((ncopies,)),
                pltpu.SemaphoreType.DMA((ncopies,)),
                pltpu.SemaphoreType.REGULAR,
            ],
            compiler_params=pltpu.CompilerParams(collective_id=0, has_side_effects=True,
                                                 vmem_limit_bytes=67043328),
            name='scmoe',
        )(h0, jnp.swapaxes(idx, 1, 2), jnp.swapaxes(slot, 1, 2), na, nf, nm,
          jnp.asarray(cos2), jnp.asarray(sin2), wr, wq, wk, wv, wo.reshape(8, QT, D),
          w1, w3, w2.reshape(8, FE, D), ue1, ue3, ue2)

    rows = P(('dp', 'ep'))
    in_specs = (rows,) * 3 + (P(),) * 11 + (P('ep'),) * 3
    return jax.shard_map(local, mesh=mesh, in_specs=in_specs, out_specs=rows, check_vma=False)
```

```python
import functools

import jax
import jax.numpy as jnp
import numpy as np
from jax import lax
from jax.experimental import pallas as pl
from jax.experimental.pallas import tpu as pltpu
from jax.sharding import PartitionSpec as P

MESH = pl.DeviceIdType.MESH
HEAD = 128
EPS = 1e-6
ROPE_BASE = 10000.0

T, D, FE, FF, TOP, CAP = 128, 2048, 768, 6144, 8, 16
EL = 16
QT = 512
CW = 512
NC = D // CW
HW = CW // 2
NS = 8
E2 = 2 * FE
KH = D // 2
NQ = 8
Q_FWD = 1
E_FWD = (0, 2, 4)
EARLY = 6
PLACE = (0, 2, 3, 6, 1, 4, 5, 7)
NF = FF // FE
T_Q = 2
T_EXP = T_Q + NQ
T_E2 = T_EXP + 2 * EL
T_WO = T_E2 + 8 * NC
T_FFN = T_WO + 2 * NC
T_W2 = T_FFN + 2 * NF
T_END = T_W2 + 3 * NC
RC = 16 * NC
R1 = RC + 8 * NC
R2 = R1 + 4 * NC
NBLK = R2 + 2 * NC

f32, bf16 = jnp.float32, jnp.bfloat16


def _dot(a, b):
    return jnp.dot(a, b, preferred_element_type=f32)


def _mult(v):
    return v if isinstance(v, int) else pl.multiple_of(v, 256)


def _kernel(h0, idx, slot, na, nf, nm, cos, sin, wr, wq, wk, wv, wo, w1, w3, w2, ue1, ue3, ue2, out,
            xz, ar, fs, qa, qb, u, info, ws, ds, x, kk, vv, g, big, ring,
            sem, send, recv, ready):
    dp, ep = lax.axis_index('dp'), lax.axis_index('ep')
    px = (dp, lax.rem(ep + 2, 4))
    py = (1 - dp, ep)
    pc = (dp, ep + 1 - 2 * lax.rem(ep, 2))
    e0 = dp * EL

    def start(t, lo=0, hi=T_END, par=None):
        s = t % NS

        def tile(src, rows=2048, at=0, width=CW):
            pltpu.make_async_copy(src, ring.at[s, pl.ds(at, rows), pl.ds(0, width)], sem.at[s]).start()

        def q(k):
            tile(wq.at[:, pl.ds(_mult(k * QT), QT)])

        def experts(k):
            first = k < EL
            e = e0 + jnp.where(first, k, 2 * EL - 1 - k)
            rows = pl.ds(_mult(jnp.where(first, 0, KH)), KH)
            tile(ue1.at[e, rows, :], KH, 0, FE)
            tile(ue3.at[e, rows, :], KH, KH, FE)

        def e2(k):
            tile(ue2.at[pl.ds(_mult(e0 * FE + k % 8 * E2), E2), pl.ds(_mult(k // 8 * CW), CW)], E2)

        def out_proj(k):
            tile(wo.at[pl.ds(_mult(k % 2 * 2048), 2048), pl.ds(_mult(k // 2 * CW), CW)])

        def up(k):
            tile(w1.at[:, pl.ds(_mult(k // 2 * FE), FE)], width=FE)

        def gate(k):
            tile(w3.at[:, pl.ds(_mult(k // 2 * FE), FE)], width=FE)

        def down(k):
            tile(w2.at[pl.ds(_mult(k % 3 * 2048), 2048), pl.ds(_mult(k // 3 * CW), CW)])

        for first, last, fns in ((T_Q, T_EXP, (q,)), (T_EXP, T_E2, (experts,)), (T_E2, T_WO, (e2,)),
                                 (T_WO, T_FFN, (out_proj,)), (T_FFN, T_W2, (up, gate)), (T_W2, T_END, (down,))):
            a, b = max(first, lo), min(last, hi)
            if a >= b:
                continue
            for p, fn in enumerate(fns):
                if isinstance(t, int):
                    if a <= t < b and (t - first) % len(fns) == p:
                        fn(t - first)
                elif (a, b) == (lo, hi) and (len(fns) == 1 or par is not None):
                    if len(fns) == 1 or p == par:
                        fn(t - first)
                else:
                    cond = (t >= a) & (t < b)
                    if len(fns) > 1:
                        cond = cond & ((t - first) % len(fns) == p)

                    @pl.when(cond)
                    def _():
                        fn(t - first)

    def wait(t, rows=2048, width=CW):
        s = t % NS
        pltpu.make_async_copy(w1.at[pl.ds(0, rows), pl.ds(0, width)], ring.at[s, pl.ds(0, rows), pl.ds(0, width)],
                              sem.at[s]).wait()
        return s

    specs = {}

    def rdma(key, src, dst, to):
        i = specs.setdefault(key, len(specs))
        return pltpu.make_async_remote_copy(src_ref=src, dst_ref=dst, send_sem=send.at[i], recv_sem=recv.at[i],
                                            device_id=to, device_id_type=MESH)

    ag = {
        'ix': lambda: rdma('ix', info.at[0], info.at[2], px),
        'iy': lambda: rdma('iy', info.at[0], info.at[3], py),
        'id': lambda: rdma('id', info.at[2], info.at[6], py),
        'ic': lambda: rdma('ic', info.at[0], info.at[1], pc),
        'c0': lambda: rdma('c0', u.at[0, pl.ds(0, 2)], u.at[1, pl.ds(0, 2)], pc),
        'c1': lambda: rdma('c1', u.at[0, pl.ds(2, 2)], u.at[1, pl.ds(2, 2)], pc),
        'x0': lambda: rdma('x0', u.at[0, 0], u.at[2, 0], px),
        'y0': lambda: rdma('y0', u.at[0, 0], u.at[3, 0], py),
        'x1': lambda: rdma('x1', u.at[0, 1], u.at[2, 1], px),
        'y1': lambda: rdma('y1', u.at[0, 1], u.at[3, 1], py),
        'x2': lambda: rdma('x2', u.at[0, 2], u.at[2, 2], px),
        'y2': lambda: rdma('y2', u.at[0, 2], u.at[3, 2], py),
        'x3': lambda: rdma('x3', u.at[0, 3], u.at[2, 3], px),
        'y3': lambda: rdma('y3', u.at[0, 3], u.at[3, 3], py),
        'd0': lambda: rdma('d0', u.at[2, 0], u.at[6, 0], py),
        'd1': lambda: rdma('d1', u.at[3, 1], u.at[6, 1], px),
        'd2': lambda: rdma('d2', u.at[2, 2], u.at[6, 2], py),
        'd3': lambda: rdma('d3', u.at[3, 3], u.at[6, 3], px),
        'cx0': lambda: rdma('cx0', u.at[2, pl.ds(0, 2)], u.at[4, pl.ds(0, 2)], pc),
        'cx1': lambda: rdma('cx1', u.at[2, pl.ds(2, 2)], u.at[4, pl.ds(2, 2)], pc),
        'cy0': lambda: rdma('cy0', u.at[3, pl.ds(0, 2)], u.at[5, pl.ds(0, 2)], pc),
        'cy1': lambda: rdma('cy1', u.at[3, pl.ds(2, 2)], u.at[5, pl.ds(2, 2)], pc),
        'cd0': lambda: rdma('cd0', u.at[6, pl.ds(0, 2)], u.at[7, pl.ds(0, 2)], pc),
        'cd1': lambda: rdma('cd1', u.at[6, pl.ds(2, 2)], u.at[7, pl.ds(2, 2)], pc),
        'icx': lambda: rdma('icx', info.at[2], info.at[4], pc),
        'icy': lambda: rdma('icy', info.at[3], info.at[5], pc),
        'icd': lambda: rdma('icd', info.at[6], info.at[7], pc),
    }
    for key in ag:
        specs.setdefault(key, len(specs))

    def sums(c, q, half=0):
        return c * 16 + q * 2 + half

    def rs(name, c):
        key = (name, c)
        if name[0] == 'c':
            n = int(name[1])
            return rdma(key, big.at[pl.ds(sums(c, 4 + n), 2)], big.at[pl.ds(RC + c * 8 + n * 2, 2)], pc)
        src, dst, to = {
            'xa': (sums(c, 1, 0), R1 + c * 4, px),
            'xb': (sums(c, 3, 0), R1 + c * 4 + 1, px),
            'ya': (sums(c, 2, 1), R1 + c * 4 + 2, py),
            'yb': (sums(c, 3, 1), R1 + c * 4 + 3, py),
            'y2': (sums(c, 2, 0), R2 + c * 2, py),
            'x2': (sums(c, 1, 1), R2 + c * 2 + 1, px),
        }[name]
        return rdma(key, big.at[src], big.at[dst], to)

    def rs_first(c, qs):
        for q in qs:
            rs('c%d' % q, c).wait_recv()
            for half in range(2):
                k = sums(c, q, half)
                big[k] = big[k] + big[RC + c * 8 + q * 2 + half]
            for name in ((), ('xa',), ('ya',), ('xb', 'yb'))[q]:
                rs(name, c).start()

    def rs_second(c):
        rs('xb', c).wait_recv()
        big[sums(c, 2, 0)] = big[sums(c, 2, 0)] + big[R1 + c * 4 + 1]
        rs('y2', c).start()
        rs('yb', c).wait_recv()
        big[sums(c, 1, 1)] = big[sums(c, 1, 1)] + big[R1 + c * 4 + 3]
        rs('x2', c).start()

    def rs_last(c, f):
        rs('xa', c).wait_recv()
        rs('y2', c).wait_recv()
        m = (big[sums(c, 0, 0)] + big[R1 + c * 4]) + big[R2 + c * 2]
        out[0, :, c * CW:c * CW + HW] = (f[:, :HW] + m).astype(bf16)
        rs('ya', c).wait_recv()
        rs('x2', c).wait_recv()
        m = (big[sums(c, 0, 1)] + big[R1 + c * 4 + 2]) + big[R2 + c * 2 + 1]
        out[0, :, c * CW + HW:(c + 1) * CW] = (f[:, HW:] + m).astype(bf16)

    barrier = pltpu.get_barrier_semaphore()
    for to in (px, py, pc):
        pl.semaphore_signal(barrier, inc=1, device_id=to, device_id_type=MESH)
    for i, src in enumerate((wk, wv)):
        pltpu.make_async_copy(src, ring.at[i, :, pl.ds(0, QT)], sem.at[i]).start()
    for t in range(T_Q, NS):
        start(t, T_Q, NS)

    def norms(i, _):
        rows = pl.ds(pl.multiple_of(i * 16, 16), 16)
        xf = h0[0, rows, :].astype(f32)
        xr = xf * lax.rsqrt(jnp.mean(xf * xf, axis=-1, keepdims=True) + EPS)
        un = (xr * nm[...].astype(f32)[None, :]).astype(bf16)
        for k in range(4):
            u[0, k, rows, :] = un[:, k * 512:(k + 1) * 512]
        xz[rows, :] = (xr * na[...].astype(f32)[None, :]).astype(bf16)
        return 0

    lax.fori_loop(0, T // 16, norms, 0, unroll=4)
    pl.semaphore_wait(barrier, 3)
    for key in ('x0', 'y1', 'c0'):
        ag[key]().start()

    logits = _dot(u[0, 0], wr[pl.ds(0, 512), :])
    for k in range(1, 4):
        logits = logits + _dot(u[0, k], wr[pl.ds(k * 512, 512), :])
    lt = logits.T
    idt = idx[0].astype(f32)
    slt = slot[0].astype(f32)
    ex = lax.broadcasted_iota(jnp.int32, (T, T), 0).astype(f32)
    sel = jnp.concatenate(
        [jnp.sum(jnp.where(ex == idt[j:j + 1, :], lt, 0.0), axis=0, keepdims=True) for j in range(TOP)], axis=0)
    gate = jnp.exp(sel - jnp.max(sel, axis=0, keepdims=True))
    gate = gate / jnp.sum(gate, axis=0, keepdims=True)
    info[0, pl.ds(0, TOP), :] = idt * float(CAP) + slt
    info[0, pl.ds(TOP, TOP), :] = gate
    for key in ('ix', 'iy', 'ic', 'x1', 'y0', 'c1'):
        ag[key]().start()

    cs, sn = cos[...], sin[...]

    def rope(v):
        return (v * cs + pltpu.roll(v, HEAD // 2, 1) * sn).astype(bf16)

    wait(0)
    wait(1)
    kf = _dot(xz[...], ring[0, :, pl.ds(0, QT)])
    vf = _dot(xz[...], ring[1, :, pl.ds(0, QT)])
    for n in range(4):
        kk[n] = rope(kf[:, n * HEAD:(n + 1) * HEAD])
        vv[n] = vf[:, n * HEAD:(n + 1) * HEAD].astype(bf16)
    start(NS, T_Q, T_E2)
    start(NS + 1, T_Q, T_E2)
    causal = lax.broadcasted_iota(jnp.int32, (T, T), 0) >= lax.broadcasted_iota(jnp.int32, (T, T), 1)

    def q_dot(s, dst):
        dst[...] = _dot(xz[...], ring[s, :, pl.ds(0, QT)])

    def q_heads(i, src):
        kg, vg = kk[i // 2], vv[i // 2]
        qs = jnp.concatenate([rope(src[:, n * HEAD:(n + 1) * HEAD]) for n in range(4)], axis=0)
        sc = lax.dot_general(qs, kg, (((1,), (1,)), ((), ())), preferred_element_type=f32) * HEAD ** -0.5
        ps = []
        for n in range(4):
            sm = jnp.where(causal, sc[n * T:(n + 1) * T], -jnp.inf)
            p = jnp.exp(sm - jnp.max(sm, axis=-1, keepdims=True))
            ps.append((p * (1.0 / jnp.sum(p, axis=-1, keepdims=True))).astype(bf16))
        o = _dot(jnp.concatenate(ps, axis=0), vg)
        for n in range(4):
            g[:, pl.ds(_mult(i * QT) + n * HEAD, HEAD)] = o[n * T:(n + 1) * T].astype(bf16)

    def q_pair(k, _):
        t = T_Q + 2 * k + 1
        s = wait(t), wait(t + 1)
        q_dot(s[0], qb)
        start(t + NS, T_EXP, T_E2)
        q_heads(2 * k, qa)
        q_dot(s[1], qa)
        start(t + 1 + NS, T_EXP, T_E2)
        q_heads(2 * k + 1, qb)

        @pl.when(k == Q_FWD)
        def _():
            ag['ix']().wait_recv()
            ag['id']().start()
            ag['x0']().wait_recv()
            ag['d0']().start()
            ag['y1']().wait_recv()
            ag['d1']().start()
            for key in ('x2', 'y3', 'x3', 'y2'):
                ag[key]().start()

        return 0

    q_dot(wait(T_Q), qa)
    start(T_Q + NS, T_EXP, T_E2)
    lax.fori_loop(0, NQ // 2 - 1, q_pair, 0)
    s_last = wait(T_EXP - 1)
    q_dot(s_last, qb)
    q_heads(NQ - 2, qa)
    q_heads(NQ - 1, qb)
    start(T_EXP - 1 + NS, T_EXP, T_E2)
    for key in ('iy', 'id', 'x1', 'y0'):
        ag[key]().wait_recv()
    for key in ('icx', 'icy', 'icd', 'cx0', 'cy0'):
        ag[key]().start()

    base = ((ep * 32 + e0) * CAP).astype(f32)

    def weights(r):
        for half in range(2):
            row = lax.broadcasted_iota(jnp.int32, (T, T), 0).astype(f32) + (base + float(half * T))
            w = jnp.zeros((T, T), f32)
            d = jnp.zeros((T, T), f32)
            for j in range(TOP):
                hit = row == info[r, pl.ds(j, 1), :]
                w = jnp.where(hit, info[r, pl.ds(TOP + j, 1), :], w)
                d = jnp.where(hit, 1.0, d)
            wt = w.T
            hi = wt.astype(bf16)
            rest = wt - hi.astype(f32)
            mid = rest.astype(bf16)
            low = (rest - mid.astype(f32)).astype(bf16)
            for n, part in enumerate((hi, mid, low)):
                ws[r, pl.ds(n * T, T), half * T:(half + 1) * T] = part
            ds[r, pl.ds(half * T, T), :] = d.astype(bf16)

    def rows_of(r, k):
        rows = _dot(ds[r], u[r, k]).astype(bf16)
        x[:, pl.ds(pl.multiple_of(r * CAP, CAP), CAP), k * 512:(k + 1) * 512] = rows.reshape(EL, CAP, 512)

    def build(r, _):
        weights(r)
        for k in range(2):
            rows_of(r, k)
        return 0

    for key in ('ic', 'c0'):
        ag[key]().wait_recv()
    lax.fori_loop(0, 4, build, 0)
    for key in ('d0', 'd1'):
        ag[key]().wait_recv()
    ag['cd0']().start()
    for key in ('icx', 'icy', 'icd', 'cx0', 'cy0'):
        ag[key]().wait_recv()
    lax.fori_loop(4, 7, build, 0)
    ag['cd0']().wait_recv()
    build(7, 0)

    def products(lhs, s):
        ha = _dot(lhs, ring[s, pl.ds(0, KH), :])
        hc = _dot(lhs, ring[s, pl.ds(KH, KH), :])
        return [h[:, j * HW:(j + 1) * HW] for h in (ha, hc) for j in range(3)]

    def first_half(i, _):
        t = T_EXP + 2 * i
        slots = [wait(t + k, width=FE) for k in range(2)]
        for k in range(2):
            e = 2 * i + k
            for j, h in enumerate(products(x[e, :, :KH], slots[k])):
                big[e * 6 + j] = h
            start(t + k + NS, T_EXP + NS, T_E2)

    def first_early(i, _):
        first_half(i, 0)

        @pl.when(i == E_FWD[0])
        def _():
            ag['x2']().wait_recv()
            ag['d2']().start()
            ag['y3']().wait_recv()
            ag['d3']().start()

        @pl.when(i == E_FWD[1])
        def _():
            for key in ('x3', 'y2'):
                ag[key]().wait_recv()
            for key in ('cx1', 'cy1'):
                ag[key]().start()

        @pl.when(i == E_FWD[2])
        def _():
            for key in ('d2', 'd3'):
                ag[key]().wait_recv()
            ag['cd1']().start()
        return 0

    def first_late(i, _):
        first_half(i, 0)
        for k in range(2, 4):
            for j in range(4):
                rows_of(4 * (i - EARLY) + j, k)
        return 0

    lax.fori_loop(0, EARLY, first_early, 0)
    for key in ('c1', 'cx1', 'cy1', 'cd1'):
        ag[key]().wait_recv()
    lax.fori_loop(EARLY, 8, first_late, 0)

    def second_half(lo, hi):
        def step(i, _):
            t = T_EXP + EL + 2 * i
            slots = [wait(t + k, width=FE) for k in range(2)]
            for k in range(2):
                e = EL - 1 - (2 * i + k)
                hs = [h + big[e * 6 + j] for j, h in enumerate(products(x[e, :, KH:], slots[k]))]
                start(t + k + NS, lo, hi)
                for j in range(3):
                    x[e, :, j * HW:(j + 1) * HW] = (hs[j] * jax.nn.sigmoid(hs[j]) * hs[3 + j]).astype(bf16)
            return 0
        return step

    turn = (EL - NS) // 2
    lax.fori_loop(0, turn, second_half(T_EXP + EL + NS, T_E2), 0)
    if (EL - NS) % 2:
        second_half(0, T_END)(turn, 0)
        turn += 1
    lax.fori_loop(turn, EL // 2, second_half(T_E2, T_WO), 0)
    pl.semaphore_signal(ready, inc=1, device_id=pc, device_id_type=MESH)

    YC = 1024

    def chunk(c):
        def part(k):
            t = T_E2 + 8 * c + 4 * k
            slots = [wait(t + j, E2) for j in range(4)]
            for j in range(4):
                for i in range(2):
                    e = 8 * k + 2 * j + i
                    x[e, :, YC:YC + CW] = _dot(x[e, :, :FE], ring[slots[j], pl.ds(i * FE, FE), pl.ds(0, CW)]).astype(bf16)
                start(t + j + NS)

        part(0)
        if c > 0:
            rs_first(c - 1, (1, 2, 0))
        part(1)
        if c == 0:
            pl.semaphore_wait(ready, 1)
        if c == 2:
            rs_second(0)

        for q in (7, 5, 6, 4, 3, 1, 2, 0):
            r = PLACE[q]
            yr = x[:, r * CAP:(r + 1) * CAP, YC:YC + CW].reshape(2 * T, CW)
            three = _dot(ws[r], yr)
            m = (three[:T] + three[T:2 * T]) + three[2 * T:]
            big[sums(c, q, 0)] = m[:, :HW]
            big[sums(c, q, 1)] = m[:, HW:]
            if q >= 4:
                rs('c%d' % (q - 4), c).start()
        rs_first(c, (3,))

    for c in range(NC):
        chunk(c)

    for n in range(D // CW):
        cols = slice(n * CW, (n + 1) * CW)
        t = T_WO + 2 * n
        s0, s1 = wait(t), wait(t + 1)
        prod = _dot(g[:, :2048], ring[s0, :, pl.ds(0, CW)])
        start(t + NS)
        prod = prod + _dot(g[:, 2048:4096], ring[s1, :, pl.ds(0, CW)])
        start(t + 1 + NS)
        ar[:, cols] = (h0[0, :, cols].astype(f32) + prod).astype(bf16)
        if n == 0:
            rs_first(NC - 1, (1, 2, 0))
            rs_second(1)

    def znorm(i, _):
        rows = pl.ds(pl.multiple_of(i * 16, 16), 16)
        xf = ar[rows, :].astype(f32)
        xr = xf * lax.rsqrt(jnp.mean(xf * xf, axis=-1, keepdims=True) + EPS)
        xz[rows, :] = (xr * nf[...].astype(f32)[None, :]).astype(bf16)
        return 0

    lax.fori_loop(0, T // 16, znorm, 0, unroll=4)

    def ffn(lo, hi):
        def step(i, _):
            t = T_FFN + 4 * i
            slots = [wait(t + k, width=FE) for k in range(4)]
            for k in range(2):
                h1 = _dot(xz[...], ring[slots[2 * k]])
                start(t + 2 * k + NS, lo, hi, NS % 2)
                h3 = _dot(xz[...], ring[slots[2 * k + 1]])
                start(t + 2 * k + 1 + NS, lo, hi, (NS + 1) % 2)
                g[:, pl.ds(_mult(i * 2 * FE) + k * FE, FE)] = (h1 * jax.nn.sigmoid(h1) * h3).astype(bf16)
            return 0
        return step

    turn = (2 * NF - NS) // 4
    lax.fori_loop(0, turn, ffn(T_FFN + NS, T_W2), 0)
    rs_second(2)
    if (2 * NF - NS) % 4:
        ffn(0, T_END)(turn, 0)
        turn += 1
    lax.fori_loop(turn, NF // 2, ffn(T_W2, T_END), 0)
    rs_second(3)

    for n in range(D // CW):
        cols = slice(n * CW, (n + 1) * CW)
        t = T_W2 + 3 * n
        slots = [wait(t + k) for k in range(3)]
        prod = None
        for k in range(3):
            term = _dot(g[:, k * 2048:(k + 1) * 2048], ring[slots[k], :, pl.ds(0, CW)])
            prod = term if prod is None else prod + term
            start(t + k + NS, T_W2, T_END)
        if n == 0:
            fs[...] = ar[:, cols].astype(f32) + prod
            continue
        if n == 1:
            rs_last(0, fs[...])
        rs_last(n, ar[:, cols].astype(f32) + prod)

    for key in ag:
        ag[key]().wait_send()
    for c in range(NC):
        for name in ('c0', 'c1', 'c2', 'c3', 'xa', 'xb', 'ya', 'yb', 'y2', 'x2'):
            rs(name, c).wait_send()


def solution(mesh):
    ang = (np.arange(T, dtype=np.float32)[:, None]
           * (ROPE_BASE ** (-2.0 * np.arange(HEAD // 2) / HEAD)).astype(np.float32)[None, :])
    cos = np.cos(ang.astype(np.float64)).astype(np.float32)
    sin = np.sin(ang.astype(np.float64)).astype(np.float32)
    cos2 = np.concatenate([cos, cos], axis=1)
    sin2 = np.concatenate([-sin, sin], axis=1)
    ncopies = 27 + 10 * NC

    def local(h0, idx, slot, na, wq, wk, wv, wo, nf, w1, w3, w2, nm, wr, ue1, ue3, ue2):
        vm = pl.BlockSpec(memory_space=pltpu.VMEM)
        hb = pl.BlockSpec(memory_space=pl.ANY)
        return pl.pallas_call(
            _kernel,
            out_shape=jax.ShapeDtypeStruct(h0.shape, bf16),
            in_specs=[vm] * 9 + [hb] * 10,
            out_specs=vm,
            scratch_shapes=[
                pltpu.VMEM((T, D), bf16),
                pltpu.VMEM((T, D), bf16),
                pltpu.VMEM((T, CW), f32),
                pltpu.VMEM((T, QT), f32),
                pltpu.VMEM((T, QT), f32),
                pltpu.VMEM((8, 4, T, D // 4), bf16),
                pltpu.VMEM((8, 2 * TOP, T), f32),
                pltpu.VMEM((8, 3 * T, 2 * T), bf16),
                pltpu.VMEM((8, 2 * T, T), bf16),
                pltpu.VMEM((EL, T, D), bf16),
                pltpu.VMEM((4, T, HEAD), bf16),
                pltpu.VMEM((4, T, HEAD), bf16),
                pltpu.VMEM((T, FF), bf16),
                pltpu.VMEM((NBLK, T, HW), f32),
                pltpu.VMEM((NS, 2048, FE), bf16),
                pltpu.SemaphoreType.DMA((NS,)),
                pltpu.SemaphoreType.DMA((ncopies,)),
                pltpu.SemaphoreType.DMA((ncopies,)),
                pltpu.SemaphoreType.REGULAR,
            ],
            compiler_params=pltpu.CompilerParams(collective_id=0, has_side_effects=True,
                                                 vmem_limit_bytes=67043328),
            name='scmoe',
        )(h0, jnp.swapaxes(idx, 1, 2), jnp.swapaxes(slot, 1, 2), na, nf, nm,
          jnp.asarray(cos2), jnp.asarray(sin2), wr, wq, wk, wv, wo, w1, w3, w2, ue1, ue3, ue2.reshape(-1, D))

    rows = P(('dp', 'ep'))
    in_specs = (rows,) * 3 + (P(),) * 11 + (P('ep'),) * 3
    return jax.shard_map(local, mesh=mesh, in_specs=in_specs, out_specs=rows, check_vma=False)
```

```python
import functools

import jax
import jax.numpy as jnp
import numpy as np
from jax import lax
from jax.experimental import pallas as pl
from jax.experimental.pallas import tpu as pltpu
from jax.sharding import PartitionSpec as P

MESH = pl.DeviceIdType.MESH
HEAD = 128
EPS = 1e-6
ROPE_BASE = 10000.0

T, D, FE, FF, TOP, CAP = 128, 2048, 768, 6144, 8, 16
EL = 16
QT = 512
CW = 512
NC = D // CW
HW = CW // 2
NS = 8
E2 = 2 * FE
KH = D // 2
NQ = 8
NW = 1
Q_FWD = 1
E_FWD = (0, 2, 4)
EARLY = 6
PLACE = (0, 2, 3, 6, 1, 4, 5, 7)
NF = FF // FE
T_Q = 2
T_WO1 = T_Q + NQ
T_EXP = T_WO1 + 2 * NW
T_E2 = T_EXP + 2 * EL
T_WO = T_E2 + 8 * NC
T_FFN = T_WO + 2 * (NC - NW)
T_W2 = T_FFN + 2 * NF
T_END = T_W2 + 3 * NC
RC = 16 * NC
R1 = RC + 8 * NC
R2 = R1 + 4 * NC
NBLK = R2 + 2 * NC

f32, bf16 = jnp.float32, jnp.bfloat16


def _dot(a, b):
    return jnp.dot(a, b, preferred_element_type=f32)


def _mult(v):
    return v if isinstance(v, int) else pl.multiple_of(v, 256)


def _kernel(h0_h, idx_h, slot_h, na_h, nf_h, nm_h, cos_h, sin_h, wr_h, wq, wk, wv, wo, w1, w3, w2, ue1, ue3, ue2, out,
            h0, idx, slot, na, nf, nm, cos, sin, wr, sem_in, sem_out, xz, ar, fs, qa, qb, u, info, ws, ds, x, kk, vv, g, big, ring,
            sem, send, recv, ready):
    dp, ep = lax.axis_index('dp'), lax.axis_index('ep')
    px = (dp, lax.rem(ep + 2, 4))
    py = (1 - dp, ep)
    pc = (dp, ep + 1 - 2 * lax.rem(ep, 2))
    e0 = dp * EL

    def start(t, lo=0, hi=T_END, par=None):
        s = t % NS

        def tile(src, rows=2048, at=0, width=CW):
            pltpu.make_async_copy(src, ring.at[s, pl.ds(at, rows), pl.ds(0, width)], sem.at[s]).start()

        def q(k):
            tile(wq.at[:, pl.ds(_mult(k * QT), QT)])

        def experts(k):
            first = k < EL
            e = e0 + jnp.where(first, k, 2 * EL - 1 - k)
            rows = pl.ds(_mult(jnp.where(first, 0, KH)), KH)
            tile(ue1.at[e, rows, :], KH, 0, FE)
            tile(ue3.at[e, rows, :], KH, KH, FE)

        def e2(k):
            tile(ue2.at[pl.ds(_mult(e0 * FE + k % 8 * E2), E2), pl.ds(_mult(k // 8 * CW), CW)], E2)

        def out_proj(k):
            tile(wo.at[pl.ds(_mult(k % 2 * 2048), 2048), pl.ds(_mult(k // 2 * CW), CW)])

        def out_rest(k):
            out_proj(k + 2 * NW)

        def up(k):
            tile(w1.at[:, pl.ds(_mult(k // 2 * FE), FE)], width=FE)

        def gate(k):
            tile(w3.at[:, pl.ds(_mult(k // 2 * FE), FE)], width=FE)

        def down(k):
            tile(w2.at[pl.ds(_mult(k % 3 * 2048), 2048), pl.ds(_mult(k // 3 * CW), CW)])

        for first, last, fns in ((T_Q, T_WO1, (q,)), (T_WO1, T_EXP, (out_proj,)), (T_EXP, T_E2, (experts,)),
                                 (T_E2, T_WO, (e2,)), (T_WO, T_FFN, (out_rest,)), (T_FFN, T_W2, (up, gate)), (T_W2, T_END, (down,))):
            a, b = max(first, lo), min(last, hi)
            if a >= b:
                continue
            for p, fn in enumerate(fns):
                if isinstance(t, int):
                    if a <= t < b and (t - first) % len(fns) == p:
                        fn(t - first)
                elif (a, b) == (lo, hi) and (len(fns) == 1 or par is not None):
                    if len(fns) == 1 or p == par:
                        fn(t - first)
                else:
                    cond = (t >= a) & (t < b)
                    if len(fns) > 1:
                        cond = cond & ((t - first) % len(fns) == p)

                    @pl.when(cond)
                    def _():
                        fn(t - first)

    def wait(t, rows=2048, width=CW):
        s = t % NS
        pltpu.make_async_copy(w1.at[pl.ds(0, rows), pl.ds(0, width)], ring.at[s, pl.ds(0, rows), pl.ds(0, width)],
                              sem.at[s]).wait()
        return s

    specs = {}

    def rdma(key, src, dst, to):
        i = specs.setdefault(key, len(specs))
        return pltpu.make_async_remote_copy(src_ref=src, dst_ref=dst, send_sem=send.at[i], recv_sem=recv.at[i],
                                            device_id=to, device_id_type=MESH)

    ag = {
        'ix': lambda: rdma('ix', info.at[0], info.at[2], px),
        'iy': lambda: rdma('iy', info.at[0], info.at[3], py),
        'id': lambda: rdma('id', info.at[2], info.at[6], py),
        'ic': lambda: rdma('ic', info.at[0], info.at[1], pc),
        'c0': lambda: rdma('c0', u.at[0, pl.ds(0, 2)], u.at[1, pl.ds(0, 2)], pc),
        'c1': lambda: rdma('c1', u.at[0, pl.ds(2, 2)], u.at[1, pl.ds(2, 2)], pc),
        'x0': lambda: rdma('x0', u.at[0, 0], u.at[2, 0], px),
        'y0': lambda: rdma('y0', u.at[0, 0], u.at[3, 0], py),
        'x1': lambda: rdma('x1', u.at[0, 1], u.at[2, 1], px),
        'y1': lambda: rdma('y1', u.at[0, 1], u.at[3, 1], py),
        'x2': lambda: rdma('x2', u.at[0, 2], u.at[2, 2], px),
        'y2': lambda: rdma('y2', u.at[0, 2], u.at[3, 2], py),
        'x3': lambda: rdma('x3', u.at[0, 3], u.at[2, 3], px),
        'y3': lambda: rdma('y3', u.at[0, 3], u.at[3, 3], py),
        'd0': lambda: rdma('d0', u.at[2, 0], u.at[6, 0], py),
        'd1': lambda: rdma('d1', u.at[3, 1], u.at[6, 1], px),
        'd2': lambda: rdma('d2', u.at[2, 2], u.at[6, 2], py),
        'd3': lambda: rdma('d3', u.at[3, 3], u.at[6, 3], px),
        'cx0': lambda: rdma('cx0', u.at[2, pl.ds(0, 2)], u.at[4, pl.ds(0, 2)], pc),
        'cx1': lambda: rdma('cx1', u.at[2, pl.ds(2, 2)], u.at[4, pl.ds(2, 2)], pc),
        'cy0': lambda: rdma('cy0', u.at[3, pl.ds(0, 2)], u.at[5, pl.ds(0, 2)], pc),
        'cy1': lambda: rdma('cy1', u.at[3, pl.ds(2, 2)], u.at[5, pl.ds(2, 2)], pc),
        'cd0': lambda: rdma('cd0', u.at[6, pl.ds(0, 2)], u.at[7, pl.ds(0, 2)], pc),
        'cd1': lambda: rdma('cd1', u.at[6, pl.ds(2, 2)], u.at[7, pl.ds(2, 2)], pc),
        'icx': lambda: rdma('icx', info.at[2], info.at[4], pc),
        'icy': lambda: rdma('icy', info.at[3], info.at[5], pc),
        'icd': lambda: rdma('icd', info.at[6], info.at[7], pc),
    }
    for key in ag:
        specs.setdefault(key, len(specs))

    def sums(c, q, half=0):
        return c * 16 + q * 2 + half

    def rs(name, c):
        key = (name, c)
        if name[0] == 'c':
            n = int(name[1])
            return rdma(key, big.at[pl.ds(sums(c, 4 + n), 2)], big.at[pl.ds(RC + c * 8 + n * 2, 2)], pc)
        src, dst, to = {
            'xa': (sums(c, 1, 0), R1 + c * 4, px),
            'xb': (sums(c, 3, 0), R1 + c * 4 + 1, px),
            'ya': (sums(c, 2, 1), R1 + c * 4 + 2, py),
            'yb': (sums(c, 3, 1), R1 + c * 4 + 3, py),
            'y2': (sums(c, 2, 0), R2 + c * 2, py),
            'x2': (sums(c, 1, 1), R2 + c * 2 + 1, px),
        }[name]
        return rdma(key, big.at[src], big.at[dst], to)

    def rs_first(c, qs):
        for q in qs:
            rs('c%d' % q, c).wait_recv()
            for half in range(2):
                k = sums(c, q, half)
                big[k] = big[k] + big[RC + c * 8 + q * 2 + half]
            for name in ((), ('xa',), ('ya',), ('xb', 'yb'))[q]:
                rs(name, c).start()

    def rs_second(c):
        rs('xb', c).wait_recv()
        big[sums(c, 2, 0)] = big[sums(c, 2, 0)] + big[R1 + c * 4 + 1]
        rs('y2', c).start()
        rs('yb', c).wait_recv()
        big[sums(c, 1, 1)] = big[sums(c, 1, 1)] + big[R1 + c * 4 + 3]
        rs('x2', c).start()

    def result(c):
        cols = pl.ds(c * CW, CW)
        return pltpu.make_async_copy(xz.at[:, cols], out.at[0, :, cols], sem_out.at[c])

    def rs_last(c, f):
        rs('xa', c).wait_recv()
        rs('y2', c).wait_recv()
        m = (big[sums(c, 0, 0)] + big[R1 + c * 4]) + big[R2 + c * 2]
        xz[:, c * CW:c * CW + HW] = (f[:, :HW] + m).astype(bf16)
        rs('ya', c).wait_recv()
        rs('x2', c).wait_recv()
        m = (big[sums(c, 0, 1)] + big[R1 + c * 4 + 2]) + big[R2 + c * 2 + 1]
        xz[:, c * CW + HW:(c + 1) * CW] = (f[:, HW:] + m).astype(bf16)
        result(c).start()

    barrier = pltpu.get_barrier_semaphore()
    for to in (px, py, pc):
        pl.semaphore_signal(barrier, inc=1, device_id=to, device_id_type=MESH)
    loads = [pltpu.make_async_copy(src, dst, sem_in.at[i]) for i, (src, dst) in enumerate((
        (h0_h, h0), (nm_h, nm), (na_h, na), (idx_h, idx), (slot_h, slot), (wr_h, wr), (cos_h, cos), (sin_h, sin),
        (nf_h, nf)))]
    for load in loads:
        load.start()
    for i, src in enumerate((wk, wv)):
        pltpu.make_async_copy(src, ring.at[i, :, pl.ds(0, QT)], sem.at[i]).start()

    for load in loads[:3]:
        load.wait()
    for t in range(T_Q, NS):
        start(t)

    def norms(i, _):
        rows = pl.ds(pl.multiple_of(i * 16, 16), 16)
        xf = h0[0, rows, :].astype(f32)
        xr = xf * lax.rsqrt(jnp.mean(xf * xf, axis=-1, keepdims=True) + EPS)
        un = (xr * nm[...].astype(f32)[None, :]).astype(bf16)
        for k in range(4):
            u[0, k, rows, :] = un[:, k * 512:(k + 1) * 512]
        xz[rows, :] = (xr * na[...].astype(f32)[None, :]).astype(bf16)
        return 0

    lax.fori_loop(0, T // 16, norms, 0, unroll=4)
    pl.semaphore_wait(barrier, 3)
    for key in ('x0', 'y1', 'c0'):
        ag[key]().start()

    for load in loads[3:]:
        load.wait()
    logits = _dot(u[0, 0], wr[pl.ds(0, 512), :])
    for k in range(1, 4):
        logits = logits + _dot(u[0, k], wr[pl.ds(k * 512, 512), :])
    lt = logits.T
    idt = idx[0].astype(f32)
    slt = slot[0].astype(f32)
    ex = lax.broadcasted_iota(jnp.int32, (T, T), 0).astype(f32)
    sel = jnp.concatenate(
        [jnp.sum(jnp.where(ex == idt[j:j + 1, :], lt, 0.0), axis=0, keepdims=True) for j in range(TOP)], axis=0)
    gate = jnp.exp(sel - jnp.max(sel, axis=0, keepdims=True))
    gate = gate / jnp.sum(gate, axis=0, keepdims=True)
    info[0, pl.ds(0, TOP), :] = idt * float(CAP) + slt
    info[0, pl.ds(TOP, TOP), :] = gate
    for key in ('ix', 'iy', 'ic', 'x1', 'y0', 'c1'):
        ag[key]().start()

    cs, sn = cos[...], sin[...]

    def rope(v):
        return (v * cs + pltpu.roll(v, HEAD // 2, 1) * sn).astype(bf16)

    wait(0)
    wait(1)
    kf = _dot(xz[...], ring[0, :, pl.ds(0, QT)])
    vf = _dot(xz[...], ring[1, :, pl.ds(0, QT)])
    for n in range(4):
        kk[n] = rope(kf[:, n * HEAD:(n + 1) * HEAD])
        vv[n] = vf[:, n * HEAD:(n + 1) * HEAD].astype(bf16)
    start(NS)
    start(NS + 1)
    causal = lax.broadcasted_iota(jnp.int32, (T, T), 0) >= lax.broadcasted_iota(jnp.int32, (T, T), 1)

    def q_dot(s, dst):
        dst[...] = _dot(xz[...], ring[s, :, pl.ds(0, QT)])

    def q_heads(i, src):
        kg, vg = kk[i // 2], vv[i // 2]
        qs = jnp.concatenate([rope(src[:, n * HEAD:(n + 1) * HEAD]) for n in range(4)], axis=0)
        sc = lax.dot_general(qs, kg, (((1,), (1,)), ((), ())), preferred_element_type=f32) * HEAD ** -0.5
        ps = []
        for n in range(4):
            sm = jnp.where(causal, sc[n * T:(n + 1) * T], -jnp.inf)
            p = jnp.exp(sm - jnp.max(sm, axis=-1, keepdims=True))
            ps.append((p * (1.0 / jnp.sum(p, axis=-1, keepdims=True))).astype(bf16))
        o = _dot(jnp.concatenate(ps, axis=0), vg)
        for n in range(4):
            g[:, pl.ds(_mult(i * QT) + n * HEAD, HEAD)] = o[n * T:(n + 1) * T].astype(bf16)

    def q_pair(k, _):
        t = T_Q + 2 * k + 1
        s = wait(t), wait(t + 1)
        q_dot(s[0], qb)
        q_heads(2 * k, qa)
        q_dot(s[1], qa)
        q_heads(2 * k + 1, qb)
        start(t + NS, T_WO1, T_E2)
        start(t + 1 + NS, T_WO1, T_E2)

        @pl.when(k == Q_FWD)
        def _():
            ag['ix']().wait_recv()
            ag['id']().start()
            ag['x0']().wait_recv()
            ag['d0']().start()
            ag['y1']().wait_recv()
            ag['d1']().start()
            for key in ('x2', 'y3', 'x3', 'y2'):
                ag[key]().start()

        return 0

    q_dot(wait(T_Q), qa)
    start(T_Q + NS)
    lax.fori_loop(0, NQ // 2 - 1, q_pair, 0)
    s_last = wait(T_WO1 - 1)
    q_dot(s_last, qb)
    q_heads(NQ - 2, qa)
    q_heads(NQ - 1, qb)
    start(T_WO1 - 1 + NS)
    for key in ('iy', 'id', 'x1', 'y0'):
        ag[key]().wait_recv()
    for key in ('icx', 'icy', 'icd', 'cx0', 'cy0'):
        ag[key]().start()

    def wo_step(n, t):
        cols = slice(n * CW, (n + 1) * CW)
        s0, s1 = wait(t), wait(t + 1)
        prod = _dot(g[:, :2048], ring[s0, :, pl.ds(0, CW)])
        start(t + NS)
        prod = prod + _dot(g[:, 2048:4096], ring[s1, :, pl.ds(0, CW)])
        start(t + 1 + NS)
        ar[:, cols] = (h0[0, :, cols].astype(f32) + prod).astype(bf16)

    wo_step(0, T_WO1)

    base = ((ep * 32 + e0) * CAP).astype(f32)

    def weights(r):
        for half in range(2):
            row = lax.broadcasted_iota(jnp.int32, (T, T), 0).astype(f32) + (base + float(half * T))
            w = jnp.zeros((T, T), f32)
            d = jnp.zeros((T, T), f32)
            for j in range(TOP):
                hit = row == info[r, pl.ds(j, 1), :]
                w = jnp.where(hit, info[r, pl.ds(TOP + j, 1), :], w)
                d = jnp.where(hit, 1.0, d)
            wt = w.T
            hi = wt.astype(bf16)
            rest = wt - hi.astype(f32)
            mid = rest.astype(bf16)
            low = (rest - mid.astype(f32)).astype(bf16)
            for n, part in enumerate((hi, mid, low)):
                ws[r, pl.ds(n * T, T), half * T:(half + 1) * T] = part
            ds[r, pl.ds(half * T, T), :] = d.astype(bf16)

    def rows_of(r, k):
        rows = _dot(ds[r], u[r, k]).astype(bf16)
        x[:, pl.ds(pl.multiple_of(r * CAP, CAP), CAP), k * 512:(k + 1) * 512] = rows.reshape(EL, CAP, 512)

    def build(r, _):
        weights(r)
        for k in range(2):
            rows_of(r, k)
        return 0

    for key in ('ic', 'c0'):
        ag[key]().wait_recv()
    lax.fori_loop(0, 4, build, 0)
    for key in ('d0', 'd1'):
        ag[key]().wait_recv()
    ag['cd0']().start()
    for n in range(1, NW):
        wo_step(n, T_WO1 + 2 * n)
    for key in ('icx', 'icy', 'icd', 'cx0', 'cy0'):
        ag[key]().wait_recv()
    lax.fori_loop(4, 7, build, 0)
    ag['cd0']().wait_recv()
    build(7, 0)

    def products(lhs, s):
        ha = _dot(lhs, ring[s, pl.ds(0, KH), :])
        hc = _dot(lhs, ring[s, pl.ds(KH, KH), :])
        return [h[:, j * HW:(j + 1) * HW] for h in (ha, hc) for j in range(3)]

    def first_half(i, _):
        t = T_EXP + 2 * i
        slots = [wait(t + k, width=FE) for k in range(2)]
        for k in range(2):
            e = 2 * i + k
            for j, h in enumerate(products(x[e, :, :KH], slots[k])):
                big[e * 6 + j] = h
            start(t + k + NS, T_EXP + NS, T_E2)

    def first_early(i, _):
        first_half(i, 0)

        @pl.when(i == E_FWD[0])
        def _():
            ag['x2']().wait_recv()
            ag['d2']().start()
            ag['y3']().wait_recv()
            ag['d3']().start()

        @pl.when(i == E_FWD[1])
        def _():
            for key in ('x3', 'y2'):
                ag[key]().wait_recv()
            for key in ('cx1', 'cy1'):
                ag[key]().start()

        @pl.when(i == E_FWD[2])
        def _():
            for key in ('d2', 'd3'):
                ag[key]().wait_recv()
            ag['cd1']().start()
        return 0

    def first_late(i, _):
        first_half(i, 0)
        for k in range(2, 4):
            for j in range(4):
                rows_of(4 * (i - EARLY) + j, k)
        return 0

    lax.fori_loop(0, EARLY, first_early, 0)
    for key in ('c1', 'cx1', 'cy1', 'cd1'):
        ag[key]().wait_recv()
    lax.fori_loop(EARLY, 8, first_late, 0)

    def second_half(lo, hi):
        def step(i, _):
            t = T_EXP + EL + 2 * i
            slots = [wait(t + k, width=FE) for k in range(2)]
            for k in range(2):
                e = EL - 1 - (2 * i + k)
                hs = [h + big[e * 6 + j] for j, h in enumerate(products(x[e, :, KH:], slots[k]))]
                start(t + k + NS, lo, hi)
                for j in range(3):
                    x[e, :, j * HW:(j + 1) * HW] = (hs[j] * jax.nn.sigmoid(hs[j]) * hs[3 + j]).astype(bf16)
            return 0
        return step

    turn = (EL - NS) // 2
    lax.fori_loop(0, turn, second_half(T_EXP + EL + NS, T_E2), 0)
    if (EL - NS) % 2:
        second_half(0, T_END)(turn, 0)
        turn += 1
    lax.fori_loop(turn, EL // 2, second_half(T_E2, T_WO), 0)
    pl.semaphore_signal(ready, inc=1, device_id=pc, device_id_type=MESH)

    YC = 1024

    def chunk(c):
        def part(k):
            t = T_E2 + 8 * c + 4 * k
            slots = [wait(t + j, E2) for j in range(4)]
            for j in range(4):
                for i in range(2):
                    e = 8 * k + 2 * j + i
                    x[e, :, YC:YC + CW] = _dot(x[e, :, :FE], ring[slots[j], pl.ds(i * FE, FE), pl.ds(0, CW)]).astype(bf16)
                start(t + j + NS)

        part(0)
        if c > 0:
            rs_first(c - 1, (1, 2, 0))
        part(1)
        if c == 0:
            pl.semaphore_wait(ready, 1)
        if c == 2:
            rs_second(0)

        for q in (7, 5, 6, 4, 3, 1, 2, 0):
            r = PLACE[q]
            yr = x[:, r * CAP:(r + 1) * CAP, YC:YC + CW].reshape(2 * T, CW)
            three = _dot(ws[r], yr)
            m = (three[:T] + three[T:2 * T]) + three[2 * T:]
            big[sums(c, q, 0)] = m[:, :HW]
            big[sums(c, q, 1)] = m[:, HW:]
            if q >= 4:
                rs('c%d' % (q - 4), c).start()
        rs_first(c, (3,))

    for c in range(NC):
        chunk(c)

    for n in range(NW, NC):
        wo_step(n, T_WO + 2 * (n - NW))
        if n == NW:
            rs_first(NC - 1, (1, 2, 0))
            rs_second(1)

    def znorm(i, _):
        rows = pl.ds(pl.multiple_of(i * 16, 16), 16)
        xf = ar[rows, :].astype(f32)
        xr = xf * lax.rsqrt(jnp.mean(xf * xf, axis=-1, keepdims=True) + EPS)
        xz[rows, :] = (xr * nf[...].astype(f32)[None, :]).astype(bf16)
        return 0

    lax.fori_loop(0, T // 16, znorm, 0, unroll=4)

    def ffn(lo, hi):
        def step(i, _):
            t = T_FFN + 4 * i
            slots = [wait(t + k, width=FE) for k in range(4)]
            for k in range(2):
                h1 = _dot(xz[...], ring[slots[2 * k]])
                start(t + 2 * k + NS, lo, hi, NS % 2)
                h3 = _dot(xz[...], ring[slots[2 * k + 1]])
                start(t + 2 * k + 1 + NS, lo, hi, (NS + 1) % 2)
                g[:, pl.ds(_mult(i * 2 * FE) + k * FE, FE)] = (h1 * jax.nn.sigmoid(h1) * h3).astype(bf16)
            return 0
        return step

    turn = (2 * NF - NS) // 4
    lax.fori_loop(0, turn, ffn(T_FFN + NS, T_W2), 0)
    rs_second(2)
    if (2 * NF - NS) % 4:
        ffn(0, T_END)(turn, 0)
        turn += 1
    lax.fori_loop(turn, NF // 2, ffn(T_W2, T_END), 0)
    rs_second(3)

    for n in range(D // CW):
        cols = slice(n * CW, (n + 1) * CW)
        t = T_W2 + 3 * n
        batch = n < NC - 1
        slots = [wait(t + k) for k in range(3)] if batch else None
        prod = None
        for k in range(3):
            s = slots[k] if batch else wait(t + k)
            term = _dot(g[:, k * 2048:(k + 1) * 2048], ring[s, :, pl.ds(0, CW)])
            prod = term if prod is None else prod + term
            start(t + k + NS, T_W2, T_END)
        if n == 0:
            fs[...] = ar[:, cols].astype(f32) + prod
            continue
        if n == 1:
            rs_last(0, fs[...])
        rs_last(n, ar[:, cols].astype(f32) + prod)

    for key in ag:
        ag[key]().wait_send()
    for c in range(NC):
        for name in ('c0', 'c1', 'c2', 'c3', 'xa', 'xb', 'ya', 'yb', 'y2', 'x2'):
            rs(name, c).wait_send()
        result(c).wait()


def solution(mesh):
    ang = (np.arange(T, dtype=np.float32)[:, None]
           * (ROPE_BASE ** (-2.0 * np.arange(HEAD // 2) / HEAD)).astype(np.float32)[None, :])
    cos = np.cos(ang.astype(np.float64)).astype(np.float32)
    sin = np.sin(ang.astype(np.float64)).astype(np.float32)
    cos2 = np.concatenate([cos, cos], axis=1)
    sin2 = np.concatenate([-sin, sin], axis=1)
    ncopies = 27 + 10 * NC

    def local(h0, idx, slot, na, wq, wk, wv, wo, nf, w1, w3, w2, nm, wr, ue1, ue3, ue2):
        hb = pl.BlockSpec(memory_space=pl.ANY)
        return pl.pallas_call(
            _kernel,
            out_shape=jax.ShapeDtypeStruct(h0.shape, bf16),
            in_specs=[hb] * 19,
            out_specs=hb,
            scratch_shapes=[
                pltpu.VMEM(h0.shape, bf16),
                pltpu.VMEM((1, TOP, T), jnp.int32),
                pltpu.VMEM((1, TOP, T), jnp.int32),
                pltpu.VMEM((D,), bf16),
                pltpu.VMEM((D,), bf16),
                pltpu.VMEM((D,), bf16),
                pltpu.VMEM((T, HEAD), f32),
                pltpu.VMEM((T, HEAD), f32),
                pltpu.VMEM(wr.shape, bf16),
                pltpu.SemaphoreType.DMA((9,)),
                pltpu.SemaphoreType.DMA((NC,)),
                pltpu.VMEM((T, D), bf16),
                pltpu.VMEM((T, D), bf16),
                pltpu.VMEM((T, CW), f32),
                pltpu.VMEM((T, QT), f32),
                pltpu.VMEM((T, QT), f32),
                pltpu.VMEM((8, 4, T, D // 4), bf16),
                pltpu.VMEM((8, 2 * TOP, T), f32),
                pltpu.VMEM((8, 3 * T, 2 * T), bf16),
                pltpu.VMEM((8, 2 * T, T), bf16),
                pltpu.VMEM((EL, T, D), bf16),
                pltpu.VMEM((4, T, HEAD), bf16),
                pltpu.VMEM((4, T, HEAD), bf16),
                pltpu.VMEM((T, FF), bf16),
                pltpu.VMEM((NBLK, T, HW), f32),
                pltpu.VMEM((NS, 2048, FE), bf16),
                pltpu.SemaphoreType.DMA((NS,)),
                pltpu.SemaphoreType.DMA((ncopies,)),
                pltpu.SemaphoreType.DMA((ncopies,)),
                pltpu.SemaphoreType.REGULAR,
            ],
            compiler_params=pltpu.CompilerParams(collective_id=0, has_side_effects=True,
                                                 vmem_limit_bytes=67043328),
            name='scmoe',
        )(h0, jnp.swapaxes(idx, 1, 2), jnp.swapaxes(slot, 1, 2), na, nf, nm,
          jnp.asarray(cos2), jnp.asarray(sin2), wr, wq, wk, wv, wo, w1, w3, w2, ue1, ue3, ue2.reshape(-1, D))

    rows = P(('dp', 'ep'))
    in_specs = (rows,) * 3 + (P(),) * 11 + (P('ep'),) * 3
    return jax.shard_map(local, mesh=mesh, in_specs=in_specs, out_specs=rows, check_vma=False)
```

```python
import functools

import jax
import jax.numpy as jnp
import numpy as np
from jax import lax
from jax.experimental import pallas as pl
from jax.experimental.pallas import tpu as pltpu
from jax.sharding import PartitionSpec as P

MESH = pl.DeviceIdType.MESH
HEAD = 128
EPS = 1e-6
ROPE_BASE = 10000.0

T, D, FE, FF, TOP, CAP = 128, 2048, 768, 6144, 8, 16
EL = 16
QT = 512
CW = 512
NC = D // CW
HW = CW // 2
NS = 8
E2 = 2 * FE
KH = D // 2
NQ = 8
NW = 1
Q_FWD = 1
E_FWD = (0, 2, 4)
EARLY = 6
PLACE = (0, 2, 3, 6, 1, 4, 5, 7)
NF = FF // FE
T_Q = 2
T_WO1 = T_Q + NQ
T_EXP = T_WO1 + 2 * NW
T_E2 = T_EXP + 2 * EL
T_WO = T_E2 + 8 * NC
T_FFN = T_WO + 2 * (NC - NW)
T_W2 = T_FFN + 2 * NF
T_END = T_W2 + 3 * NC
RC = 16 * NC
R1 = RC + 8 * NC
R2 = R1 + 4 * NC
NBLK = R2 + 2 * NC

f32, bf16 = jnp.float32, jnp.bfloat16


def _dot(a, b):
    return jnp.dot(a, b, preferred_element_type=f32)


def _mult(v):
    return v if isinstance(v, int) else pl.multiple_of(v, 256)


def _kernel(h0_h, idx_h, slot_h, na_h, nf_h, nm_h, cos_h, sin_h, wr_h, wq, wk, wv, wo, w1, w3, w2, ue1, ue3, ue2, out,
            h0, idx, slot, na, nf, nm, cos, sin, wr, sem_in, xz, ar, fs, qa, qb, u, info, ws, ds, x, kk, vv, g, big, ring,
            sem, send, recv, ready):
    dp, ep = lax.axis_index('dp'), lax.axis_index('ep')
    px = (dp, lax.rem(ep + 2, 4))
    py = (1 - dp, ep)
    pc = (dp, ep + 1 - 2 * lax.rem(ep, 2))
    e0 = dp * EL

    def start(t, lo=0, hi=T_END, par=None):
        s = t % NS

        def tile(src, rows=2048, at=0, width=CW):
            pltpu.make_async_copy(src, ring.at[s, pl.ds(at, rows), pl.ds(0, width)], sem.at[s]).start()

        def q(k):
            tile(wq.at[:, pl.ds(_mult(k * QT), QT)])

        def experts(k):
            first = k < EL
            e = e0 + jnp.where(first, k, 2 * EL - 1 - k)
            rows = pl.ds(_mult(jnp.where(first, 0, KH)), KH)
            tile(ue1.at[e, rows, :], KH, 0, FE)
            tile(ue3.at[e, rows, :], KH, KH, FE)

        def e2(k):
            tile(ue2.at[pl.ds(_mult(e0 * FE + k % 8 * E2), E2), pl.ds(_mult(k // 8 * CW), CW)], E2)

        def out_proj(k):
            tile(wo.at[pl.ds(_mult(k % 2 * 2048), 2048), pl.ds(_mult(k // 2 * CW), CW)])

        def out_rest(k):
            out_proj(k + 2 * NW)

        def up(k):
            tile(w1.at[:, pl.ds(_mult(k // 2 * FE), FE)], width=FE)

        def gate(k):
            tile(w3.at[:, pl.ds(_mult(k // 2 * FE), FE)], width=FE)

        def down(k):
            tile(w2.at[pl.ds(_mult(k % 3 * 2048), 2048), pl.ds(_mult(k // 3 * CW), CW)])

        for first, last, fns in ((T_Q, T_WO1, (q,)), (T_WO1, T_EXP, (out_proj,)), (T_EXP, T_E2, (experts,)),
                                 (T_E2, T_WO, (e2,)), (T_WO, T_FFN, (out_rest,)), (T_FFN, T_W2, (up, gate)), (T_W2, T_END, (down,))):
            a, b = max(first, lo), min(last, hi)
            if a >= b:
                continue
            for p, fn in enumerate(fns):
                if isinstance(t, int):
                    if a <= t < b and (t - first) % len(fns) == p:
                        fn(t - first)
                elif (a, b) == (lo, hi) and (len(fns) == 1 or par is not None):
                    if len(fns) == 1 or p == par:
                        fn(t - first)
                else:
                    cond = (t >= a) & (t < b)
                    if len(fns) > 1:
                        cond = cond & ((t - first) % len(fns) == p)

                    @pl.when(cond)
                    def _():
                        fn(t - first)

    def wait(t, rows=2048, width=CW):
        s = t % NS
        pltpu.make_async_copy(w1.at[pl.ds(0, rows), pl.ds(0, width)], ring.at[s, pl.ds(0, rows), pl.ds(0, width)],
                              sem.at[s]).wait()
        return s

    specs = {}

    def rdma(key, src, dst, to):
        i = specs.setdefault(key, len(specs))
        return pltpu.make_async_remote_copy(src_ref=src, dst_ref=dst, send_sem=send.at[i], recv_sem=recv.at[i],
                                            device_id=to, device_id_type=MESH)

    ag = {
        'ix': lambda: rdma('ix', info.at[0], info.at[2], px),
        'iy': lambda: rdma('iy', info.at[0], info.at[3], py),
        'id': lambda: rdma('id', info.at[2], info.at[6], py),
        'ic': lambda: rdma('ic', info.at[0], info.at[1], pc),
        'c0': lambda: rdma('c0', u.at[0, pl.ds(0, 2)], u.at[1, pl.ds(0, 2)], pc),
        'c1': lambda: rdma('c1', u.at[0, pl.ds(2, 2)], u.at[1, pl.ds(2, 2)], pc),
        'x0': lambda: rdma('x0', u.at[0, 0], u.at[2, 0], px),
        'y0': lambda: rdma('y0', u.at[0, 0], u.at[3, 0], py),
        'x1': lambda: rdma('x1', u.at[0, 1], u.at[2, 1], px),
        'y1': lambda: rdma('y1', u.at[0, 1], u.at[3, 1], py),
        'x2': lambda: rdma('x2', u.at[0, 2], u.at[2, 2], px),
        'y2': lambda: rdma('y2', u.at[0, 2], u.at[3, 2], py),
        'x3': lambda: rdma('x3', u.at[0, 3], u.at[2, 3], px),
        'y3': lambda: rdma('y3', u.at[0, 3], u.at[3, 3], py),
        'd0': lambda: rdma('d0', u.at[2, 0], u.at[6, 0], py),
        'd1': lambda: rdma('d1', u.at[3, 1], u.at[6, 1], px),
        'd2': lambda: rdma('d2', u.at[2, 2], u.at[6, 2], py),
        'd3': lambda: rdma('d3', u.at[3, 3], u.at[6, 3], px),
        'cx0': lambda: rdma('cx0', u.at[2, pl.ds(0, 2)], u.at[4, pl.ds(0, 2)], pc),
        'cx1': lambda: rdma('cx1', u.at[2, pl.ds(2, 2)], u.at[4, pl.ds(2, 2)], pc),
        'cy0': lambda: rdma('cy0', u.at[3, pl.ds(0, 2)], u.at[5, pl.ds(0, 2)], pc),
        'cy1': lambda: rdma('cy1', u.at[3, pl.ds(2, 2)], u.at[5, pl.ds(2, 2)], pc),
        'cd0': lambda: rdma('cd0', u.at[6, pl.ds(0, 2)], u.at[7, pl.ds(0, 2)], pc),
        'cd1': lambda: rdma('cd1', u.at[6, pl.ds(2, 2)], u.at[7, pl.ds(2, 2)], pc),
        'icx': lambda: rdma('icx', info.at[2], info.at[4], pc),
        'icy': lambda: rdma('icy', info.at[3], info.at[5], pc),
        'icd': lambda: rdma('icd', info.at[6], info.at[7], pc),
    }
    for key in ag:
        specs.setdefault(key, len(specs))

    def sums(c, q, half=0):
        return c * 16 + q * 2 + half

    def rs(name, c):
        key = (name, c)
        if name[0] == 'c':
            n = int(name[1])
            return rdma(key, big.at[pl.ds(sums(c, 4 + n), 2)], big.at[pl.ds(RC + c * 8 + n * 2, 2)], pc)
        src, dst, to = {
            'xa': (sums(c, 1, 0), R1 + c * 4, px),
            'xb': (sums(c, 3, 0), R1 + c * 4 + 1, px),
            'ya': (sums(c, 2, 1), R1 + c * 4 + 2, py),
            'yb': (sums(c, 3, 1), R1 + c * 4 + 3, py),
            'y2': (sums(c, 2, 0), R2 + c * 2, py),
            'x2': (sums(c, 1, 1), R2 + c * 2 + 1, px),
        }[name]
        return rdma(key, big.at[src], big.at[dst], to)

    def rs_first(c, qs):
        for q in qs:
            rs('c%d' % q, c).wait_recv()
            for half in range(2):
                k = sums(c, q, half)
                big[k] = big[k] + big[RC + c * 8 + q * 2 + half]
            for name in ((), ('xa',), ('ya',), ('xb', 'yb'))[q]:
                rs(name, c).start()

    def rs_second(c):
        rs('xb', c).wait_recv()
        big[sums(c, 2, 0)] = big[sums(c, 2, 0)] + big[R1 + c * 4 + 1]
        rs('y2', c).start()
        rs('yb', c).wait_recv()
        big[sums(c, 1, 1)] = big[sums(c, 1, 1)] + big[R1 + c * 4 + 3]
        rs('x2', c).start()

    def rs_last(c, f):
        rs('xa', c).wait_recv()
        rs('y2', c).wait_recv()
        m = (big[sums(c, 0, 0)] + big[R1 + c * 4]) + big[R2 + c * 2]
        out[0, :, c * CW:c * CW + HW] = (f[:, :HW] + m).astype(bf16)
        rs('ya', c).wait_recv()
        rs('x2', c).wait_recv()
        m = (big[sums(c, 0, 1)] + big[R1 + c * 4 + 2]) + big[R2 + c * 2 + 1]
        out[0, :, c * CW + HW:(c + 1) * CW] = (f[:, HW:] + m).astype(bf16)

    barrier = pltpu.get_barrier_semaphore()
    for to in (px, py, pc):
        pl.semaphore_signal(barrier, inc=1, device_id=to, device_id_type=MESH)
    loads = [pltpu.make_async_copy(src, dst, sem_in.at[i]) for i, (src, dst) in enumerate((
        (h0_h, h0), (nm_h, nm), (na_h, na), (idx_h, idx), (slot_h, slot), (wr_h, wr), (cos_h, cos), (sin_h, sin),
        (nf_h, nf)))]
    for load in loads:
        load.start()
    for i, src in enumerate((wk, wv)):
        pltpu.make_async_copy(src, ring.at[i, :, pl.ds(0, QT)], sem.at[i]).start()

    for load in loads[:3]:
        load.wait()
    for t in range(T_Q, NS):
        start(t)

    def norms(i, _):
        rows = pl.ds(pl.multiple_of(i * 16, 16), 16)
        xf = h0[0, rows, :].astype(f32)
        xr = xf * lax.rsqrt(jnp.mean(xf * xf, axis=-1, keepdims=True) + EPS)
        un = (xr * nm[...].astype(f32)[None, :]).astype(bf16)
        for k in range(4):
            u[0, k, rows, :] = un[:, k * 512:(k + 1) * 512]
        xz[rows, :] = (xr * na[...].astype(f32)[None, :]).astype(bf16)
        return 0

    lax.fori_loop(0, T // 16, norms, 0, unroll=4)
    pl.semaphore_wait(barrier, 3)
    for key in ('x0', 'y1', 'c0'):
        ag[key]().start()

    for load in loads[3:]:
        load.wait()
    logits = _dot(u[0, 0], wr[pl.ds(0, 512), :])
    for k in range(1, 4):
        logits = logits + _dot(u[0, k], wr[pl.ds(k * 512, 512), :])
    lt = logits.T
    idt = idx[0].astype(f32)
    slt = slot[0].astype(f32)
    ex = lax.broadcasted_iota(jnp.int32, (T, T), 0).astype(f32)
    sel = jnp.concatenate(
        [jnp.sum(jnp.where(ex == idt[j:j + 1, :], lt, 0.0), axis=0, keepdims=True) for j in range(TOP)], axis=0)
    gate = jnp.exp(sel - jnp.max(sel, axis=0, keepdims=True))
    gate = gate / jnp.sum(gate, axis=0, keepdims=True)
    info[0, pl.ds(0, TOP), :] = idt * float(CAP) + slt
    info[0, pl.ds(TOP, TOP), :] = gate
    for key in ('ix', 'iy', 'ic', 'x1', 'y0', 'c1'):
        ag[key]().start()

    cs, sn = cos[...], sin[...]

    def rope(v):
        return (v * cs + pltpu.roll(v, HEAD // 2, 1) * sn).astype(bf16)

    wait(0)
    wait(1)
    kf = _dot(xz[...], ring[0, :, pl.ds(0, QT)])
    vf = _dot(xz[...], ring[1, :, pl.ds(0, QT)])
    for n in range(4):
        kk[n] = rope(kf[:, n * HEAD:(n + 1) * HEAD])
        vv[n] = vf[:, n * HEAD:(n + 1) * HEAD].astype(bf16)
    start(NS)
    start(NS + 1)
    causal = lax.broadcasted_iota(jnp.int32, (T, T), 0) >= lax.broadcasted_iota(jnp.int32, (T, T), 1)

    def q_dot(s, dst):
        dst[...] = _dot(xz[...], ring[s, :, pl.ds(0, QT)])

    def q_heads(i, src):
        kg, vg = kk[i // 2], vv[i // 2]
        qs = jnp.concatenate([rope(src[:, n * HEAD:(n + 1) * HEAD]) for n in range(4)], axis=0)
        sc = lax.dot_general(qs, kg, (((1,), (1,)), ((), ())), preferred_element_type=f32) * HEAD ** -0.5
        ps = []
        for n in range(4):
            sm = jnp.where(causal, sc[n * T:(n + 1) * T], -jnp.inf)
            p = jnp.exp(sm - jnp.max(sm, axis=-1, keepdims=True))
            ps.append((p * (1.0 / jnp.sum(p, axis=-1, keepdims=True))).astype(bf16))
        o = _dot(jnp.concatenate(ps, axis=0), vg)
        for n in range(4):
            g[:, pl.ds(_mult(i * QT) + n * HEAD, HEAD)] = o[n * T:(n + 1) * T].astype(bf16)

    def q_pair(k, _):
        t = T_Q + 2 * k + 1
        s = wait(t), wait(t + 1)
        q_dot(s[0], qb)
        q_heads(2 * k, qa)
        q_dot(s[1], qa)
        q_heads(2 * k + 1, qb)
        start(t + NS, T_WO1, T_E2)
        start(t + 1 + NS, T_WO1, T_E2)

        @pl.when(k == Q_FWD)
        def _():
            ag['ix']().wait_recv()
            ag['id']().start()
            ag['x0']().wait_recv()
            ag['d0']().start()
            ag['y1']().wait_recv()
            ag['d1']().start()
            for key in ('x2', 'y3', 'x3', 'y2'):
                ag[key]().start()

        return 0

    q_dot(wait(T_Q), qa)
    start(T_Q + NS)
    lax.fori_loop(0, NQ // 2 - 1, q_pair, 0)
    s_last = wait(T_WO1 - 1)
    q_dot(s_last, qb)
    q_heads(NQ - 2, qa)
    q_heads(NQ - 1, qb)
    start(T_WO1 - 1 + NS)
    for key in ('iy', 'id', 'x1', 'y0'):
        ag[key]().wait_recv()
    for key in ('icx', 'icy', 'icd', 'cx0', 'cy0'):
        ag[key]().start()

    def wo_step(n, t):
        cols = slice(n * CW, (n + 1) * CW)
        s0, s1 = wait(t), wait(t + 1)
        prod = _dot(g[:, :2048], ring[s0, :, pl.ds(0, CW)])
        start(t + NS)
        prod = prod + _dot(g[:, 2048:4096], ring[s1, :, pl.ds(0, CW)])
        start(t + 1 + NS)
        ar[:, cols] = (h0[0, :, cols].astype(f32) + prod).astype(bf16)

    wo_step(0, T_WO1)

    base = ((ep * 32 + e0) * CAP).astype(f32)

    def weights(r):
        for half in range(2):
            row = lax.broadcasted_iota(jnp.int32, (T, T), 0).astype(f32) + (base + float(half * T))
            w = jnp.zeros((T, T), f32)
            d = jnp.zeros((T, T), f32)
            for j in range(TOP):
                hit = row == info[r, pl.ds(j, 1), :]
                w = jnp.where(hit, info[r, pl.ds(TOP + j, 1), :], w)
                d = jnp.where(hit, 1.0, d)
            wt = w.T
            hi = wt.astype(bf16)
            rest = wt - hi.astype(f32)
            mid = rest.astype(bf16)
            low = (rest - mid.astype(f32)).astype(bf16)
            for n, part in enumerate((hi, mid, low)):
                ws[r, pl.ds(n * T, T), half * T:(half + 1) * T] = part
            ds[r, pl.ds(half * T, T), :] = d.astype(bf16)

    def rows_of(r, k):
        rows = _dot(ds[r], u[r, k]).astype(bf16)
        x[:, pl.ds(pl.multiple_of(r * CAP, CAP), CAP), k * 512:(k + 1) * 512] = rows.reshape(EL, CAP, 512)

    def build(r, _):
        weights(r)
        for k in range(2):
            rows_of(r, k)
        return 0

    for key in ('ic', 'c0'):
        ag[key]().wait_recv()
    lax.fori_loop(0, 4, build, 0)
    for key in ('d0', 'd1'):
        ag[key]().wait_recv()
    ag['cd0']().start()
    for n in range(1, NW):
        wo_step(n, T_WO1 + 2 * n)
    for key in ('icx', 'icy', 'icd', 'cx0', 'cy0'):
        ag[key]().wait_recv()
    lax.fori_loop(4, 7, build, 0)
    ag['cd0']().wait_recv()
    build(7, 0)

    def products(lhs, s):
        ha = _dot(lhs, ring[s, pl.ds(0, KH), :])
        hc = _dot(lhs, ring[s, pl.ds(KH, KH), :])
        return [h[:, j * HW:(j + 1) * HW] for h in (ha, hc) for j in range(3)]

    def first_half(i, _):
        t = T_EXP + 2 * i
        slots = [wait(t + k, width=FE) for k in range(2)]
        for k in range(2):
            e = 2 * i + k
            for j, h in enumerate(products(x[e, :, :KH], slots[k])):
                big[e * 6 + j] = h
            start(t + k + NS, T_EXP + NS, T_E2)

    def first_early(i, _):
        first_half(i, 0)

        @pl.when(i == E_FWD[0])
        def _():
            ag['x2']().wait_recv()
            ag['d2']().start()
            ag['y3']().wait_recv()
            ag['d3']().start()

        @pl.when(i == E_FWD[1])
        def _():
            for key in ('x3', 'y2'):
                ag[key]().wait_recv()
            for key in ('cx1', 'cy1'):
                ag[key]().start()

        @pl.when(i == E_FWD[2])
        def _():
            for key in ('d2', 'd3'):
                ag[key]().wait_recv()
            ag['cd1']().start()
        return 0

    def first_late(i, _):
        first_half(i, 0)
        for k in range(2, 4):
            for j in range(4):
                rows_of(4 * (i - EARLY) + j, k)
        return 0

    lax.fori_loop(0, EARLY, first_early, 0)
    for key in ('c1', 'cx1', 'cy1', 'cd1'):
        ag[key]().wait_recv()
    lax.fori_loop(EARLY, 8, first_late, 0)

    def second_half(lo, hi):
        def step(i, _):
            t = T_EXP + EL + 2 * i
            slots = [wait(t + k, width=FE) for k in range(2)]
            for k in range(2):
                e = EL - 1 - (2 * i + k)
                hs = [h + big[e * 6 + j] for j, h in enumerate(products(x[e, :, KH:], slots[k]))]
                start(t + k + NS, lo, hi)
                for j in range(3):
                    x[e, :, j * HW:(j + 1) * HW] = (hs[j] * jax.nn.sigmoid(hs[j]) * hs[3 + j]).astype(bf16)
            return 0
        return step

    turn = (EL - NS) // 2
    lax.fori_loop(0, turn, second_half(T_EXP + EL + NS, T_E2), 0)
    if (EL - NS) % 2:
        second_half(0, T_END)(turn, 0)
        turn += 1
    lax.fori_loop(turn, EL // 2, second_half(T_E2, T_WO), 0)
    pl.semaphore_signal(ready, inc=1, device_id=pc, device_id_type=MESH)

    YC = 1024

    def chunk(c):
        def part(k):
            t = T_E2 + 8 * c + 4 * k
            slots = [wait(t + j, E2) for j in range(4)]
            for j in range(4):
                for i in range(2):
                    e = 8 * k + 2 * j + i
                    x[e, :, YC:YC + CW] = _dot(x[e, :, :FE], ring[slots[j], pl.ds(i * FE, FE), pl.ds(0, CW)]).astype(bf16)
                start(t + j + NS)

        part(0)
        if c > 0:
            rs_first(c - 1, (1, 2, 0))
        part(1)
        if c == 0:
            pl.semaphore_wait(ready, 1)
        if c == 2:
            rs_second(0)

        for q in (7, 5, 6, 4, 3, 1, 2, 0):
            r = PLACE[q]
            yr = x[:, r * CAP:(r + 1) * CAP, YC:YC + CW].reshape(2 * T, CW)
            three = _dot(ws[r], yr)
            m = (three[:T] + three[T:2 * T]) + three[2 * T:]
            big[sums(c, q, 0)] = m[:, :HW]
            big[sums(c, q, 1)] = m[:, HW:]
            if q >= 4:
                rs('c%d' % (q - 4), c).start()
        rs_first(c, (3,))

    for c in range(NC):
        chunk(c)

    for n in range(NW, NC):
        wo_step(n, T_WO + 2 * (n - NW))
        if n == NW:
            rs_first(NC - 1, (1, 2, 0))
            rs_second(1)

    def znorm(i, _):
        rows = pl.ds(pl.multiple_of(i * 16, 16), 16)
        xf = ar[rows, :].astype(f32)
        xr = xf * lax.rsqrt(jnp.mean(xf * xf, axis=-1, keepdims=True) + EPS)
        xz[rows, :] = (xr * nf[...].astype(f32)[None, :]).astype(bf16)
        return 0

    lax.fori_loop(0, T // 16, znorm, 0, unroll=4)

    def ffn(lo, hi):
        def step(i, _):
            t = T_FFN + 4 * i
            slots = [wait(t + k, width=FE) for k in range(4)]
            for k in range(2):
                h1 = _dot(xz[...], ring[slots[2 * k]])
                start(t + 2 * k + NS, lo, hi, NS % 2)
                h3 = _dot(xz[...], ring[slots[2 * k + 1]])
                start(t + 2 * k + 1 + NS, lo, hi, (NS + 1) % 2)
                g[:, pl.ds(_mult(i * 2 * FE) + k * FE, FE)] = (h1 * jax.nn.sigmoid(h1) * h3).astype(bf16)
            return 0
        return step

    turn = (2 * NF - NS) // 4
    lax.fori_loop(0, turn, ffn(T_FFN + NS, T_W2), 0)
    rs_second(2)
    if (2 * NF - NS) % 4:
        ffn(0, T_END)(turn, 0)
        turn += 1
    lax.fori_loop(turn, NF // 2, ffn(T_W2, T_END), 0)
    rs_second(3)

    for n in range(D // CW):
        cols = slice(n * CW, (n + 1) * CW)
        t = T_W2 + 3 * n
        batch = n < NC - 1
        slots = [wait(t + k) for k in range(3)] if batch else None
        prod = None
        for k in range(3):
            s = slots[k] if batch else wait(t + k)
            term = _dot(g[:, k * 2048:(k + 1) * 2048], ring[s, :, pl.ds(0, CW)])
            prod = term if prod is None else prod + term
            start(t + k + NS, T_W2, T_END)
        if n == 0:
            fs[...] = ar[:, cols].astype(f32) + prod
            continue
        if n == 1:
            rs_last(0, fs[...])
        rs_last(n, ar[:, cols].astype(f32) + prod)

    for key in ag:
        ag[key]().wait_send()
    for c in range(NC):
        for name in ('c0', 'c1', 'c2', 'c3', 'xa', 'xb', 'ya', 'yb', 'y2', 'x2'):
            rs(name, c).wait_send()


def solution(mesh):
    ang = (np.arange(T, dtype=np.float32)[:, None]
           * (ROPE_BASE ** (-2.0 * np.arange(HEAD // 2) / HEAD)).astype(np.float32)[None, :])
    cos = np.cos(ang.astype(np.float64)).astype(np.float32)
    sin = np.sin(ang.astype(np.float64)).astype(np.float32)
    cos2 = np.concatenate([cos, cos], axis=1)
    sin2 = np.concatenate([-sin, sin], axis=1)
    ncopies = 27 + 10 * NC

    def local(h0, idx, slot, na, wq, wk, wv, wo, nf, w1, w3, w2, nm, wr, ue1, ue3, ue2):
        hb = pl.BlockSpec(memory_space=pl.ANY)
        return pl.pallas_call(
            _kernel,
            out_shape=pltpu.VMEM(h0.shape, bf16),
            in_specs=[hb] * 19,
            out_specs=pl.BlockSpec(memory_space=pltpu.VMEM),
            scratch_shapes=[
                pltpu.VMEM(h0.shape, bf16),
                pltpu.VMEM((1, TOP, T), jnp.int32),
                pltpu.VMEM((1, TOP, T), jnp.int32),
                pltpu.VMEM((D,), bf16),
                pltpu.VMEM((D,), bf16),
                pltpu.VMEM((D,), bf16),
                pltpu.VMEM((T, HEAD), f32),
                pltpu.VMEM((T, HEAD), f32),
                pltpu.VMEM(wr.shape, bf16),
                pltpu.SemaphoreType.DMA((9,)),
                pltpu.VMEM((T, D), bf16),
                pltpu.VMEM((T, D), bf16),
                pltpu.VMEM((T, CW), f32),
                pltpu.VMEM((T, QT), f32),
                pltpu.VMEM((T, QT), f32),
                pltpu.VMEM((8, 4, T, D // 4), bf16),
                pltpu.VMEM((8, 2 * TOP, T), f32),
                pltpu.VMEM((8, 3 * T, 2 * T), bf16),
                pltpu.VMEM((8, 2 * T, T), bf16),
                pltpu.VMEM((EL, T, D), bf16),
                pltpu.VMEM((4, T, HEAD), bf16),
                pltpu.VMEM((4, T, HEAD), bf16),
                pltpu.VMEM((T, FF), bf16),
                pltpu.VMEM((NBLK, T, HW), f32),
                pltpu.VMEM((NS, 2048, FE), bf16),
                pltpu.SemaphoreType.DMA((NS,)),
                pltpu.SemaphoreType.DMA((ncopies,)),
                pltpu.SemaphoreType.DMA((ncopies,)),
                pltpu.SemaphoreType.REGULAR,
            ],
            compiler_params=pltpu.CompilerParams(collective_id=0, has_side_effects=True,
                                                 vmem_limit_bytes=66100000),
            name='scmoe',
        )(h0, jnp.swapaxes(idx, 1, 2), jnp.swapaxes(slot, 1, 2), na, nf, nm,
          jnp.asarray(cos2), jnp.asarray(sin2), wr, wq, wk, wv, wo, w1, w3, w2, ue1, ue3, ue2.reshape(-1, D))

    rows = P(('dp', 'ep'))
    in_specs = (rows,) * 3 + (P(),) * 11 + (P('ep'),) * 3
    return jax.shard_map(local, mesh=mesh, in_specs=in_specs, out_specs=rows, check_vma=False)
```

```python
import functools

import jax
import jax.numpy as jnp
import numpy as np
from jax import lax
from jax.experimental import pallas as pl
from jax.experimental.pallas import tpu as pltpu
from jax.sharding import PartitionSpec as P

MESH = pl.DeviceIdType.MESH
HEAD = 128
EPS = 1e-6
ROPE_BASE = 10000.0

T, D, FE, FF, TOP, CAP = 128, 2048, 768, 6144, 8, 16
EL = 16
QT = 512
CW = 512
NC = D // CW
HW = CW // 2
NS = 8
E2 = 2 * FE
KH = D // 2
NQ = 8
NW = 1
Q_FWD = 1
E_FWD = (0, 2, 4)
EARLY = 6
PLACE = (0, 2, 3, 6, 1, 4, 5, 7)
NF = FF // FE
T_Q = 2
T_WO1 = T_Q + NQ
T_EXP = T_WO1 + 2 * NW
T_E2 = T_EXP + 2 * EL
T_WO = T_E2 + 8 * NC
T_FFN = T_WO + 2 * (NC - NW)
T_W2 = T_FFN + 2 * NF
T_END = T_W2 + 3 * NC
RC = 16 * NC
R1 = RC + 8 * NC
R2 = R1 + 4 * NC
NBLK = R2 + 2 * NC

f32, bf16 = jnp.float32, jnp.bfloat16


def _dot(a, b):
    return jnp.dot(a, b, preferred_element_type=f32)


def _mult(v):
    return v if isinstance(v, int) else pl.multiple_of(v, 256)


def _kernel(h0_h, idx_h, slot_h, na_h, nf_h, nm_h, cos_h, sin_h, wr_h, wq, wk, wv, wo, w1, w3, w2, ue1, ue3, ue2, out,
            h0, idx, slot, na, nf, nm, cos, sin, wr, sem_in, xz, ar, fs, qa, qb, u, info, ws, ds, x, kk, vv, g, big, ring,
            sem, send, recv, ready):
    dp, ep = lax.axis_index('dp'), lax.axis_index('ep')
    px = (dp, lax.rem(ep + 2, 4))
    py = (1 - dp, ep)
    pc = (dp, ep + 1 - 2 * lax.rem(ep, 2))
    e0 = dp * EL

    def start(t, lo=0, hi=T_END, par=None):
        s = t % NS

        def tile(src, rows=2048, at=0, width=CW):
            pltpu.make_async_copy(src, ring.at[s, pl.ds(at, rows), pl.ds(0, width)], sem.at[s]).start()

        def q(k):
            tile(wq.at[:, pl.ds(_mult(k * QT), QT)])

        def experts(k):
            first = k < EL
            e = e0 + jnp.where(first, k, 2 * EL - 1 - k)
            rows = pl.ds(_mult(jnp.where(first, 0, KH)), KH)
            tile(ue1.at[e, rows, :], KH, 0, FE)
            tile(ue3.at[e, rows, :], KH, KH, FE)

        def e2(k):
            tile(ue2.at[pl.ds(_mult(e0 * FE + k % 8 * E2), E2), pl.ds(_mult(k // 8 * CW), CW)], E2)

        def out_proj(k):
            tile(wo.at[pl.ds(_mult(k % 2 * 2048), 2048), pl.ds(_mult(k // 2 * CW), CW)])

        def out_rest(k):
            out_proj(k + 2 * NW)

        def up(k):
            tile(w1.at[:, pl.ds(_mult(k // 2 * FE), FE)], width=FE)

        def gate(k):
            tile(w3.at[:, pl.ds(_mult(k // 2 * FE), FE)], width=FE)

        def down(k):
            tile(w2.at[pl.ds(_mult(k % 3 * 2048), 2048), pl.ds(_mult(k // 3 * CW), CW)])

        for first, last, fns in ((T_Q, T_WO1, (q,)), (T_WO1, T_EXP, (out_proj,)), (T_EXP, T_E2, (experts,)),
                                 (T_E2, T_WO, (e2,)), (T_WO, T_FFN, (out_rest,)), (T_FFN, T_W2, (up, gate)), (T_W2, T_END, (down,))):
            a, b = max(first, lo), min(last, hi)
            if a >= b:
                continue
            for p, fn in enumerate(fns):
                if isinstance(t, int):
                    if a <= t < b and (t - first) % len(fns) == p:
                        fn(t - first)
                elif (a, b) == (lo, hi) and (len(fns) == 1 or par is not None):
                    if len(fns) == 1 or p == par:
                        fn(t - first)
                else:
                    cond = (t >= a) & (t < b)
                    if len(fns) > 1:
                        cond = cond & ((t - first) % len(fns) == p)

                    @pl.when(cond)
                    def _():
                        fn(t - first)

    def wait(t, rows=2048, width=CW):
        s = t % NS
        pltpu.make_async_copy(w1.at[pl.ds(0, rows), pl.ds(0, width)], ring.at[s, pl.ds(0, rows), pl.ds(0, width)],
                              sem.at[s]).wait()
        return s

    specs = {}

    def rdma(key, src, dst, to):
        i = specs.setdefault(key, len(specs))
        return pltpu.make_async_remote_copy(src_ref=src, dst_ref=dst, send_sem=send.at[i], recv_sem=recv.at[i],
                                            device_id=to, device_id_type=MESH)

    ag = {
        'ix': lambda: rdma('ix', info.at[0], info.at[2], px),
        'iy': lambda: rdma('iy', info.at[0], info.at[3], py),
        'id': lambda: rdma('id', info.at[2], info.at[6], py),
        'ic': lambda: rdma('ic', info.at[0], info.at[1], pc),
        'c0': lambda: rdma('c0', u.at[0, pl.ds(0, 2)], u.at[1, pl.ds(0, 2)], pc),
        'c1': lambda: rdma('c1', u.at[0, pl.ds(2, 2)], u.at[1, pl.ds(2, 2)], pc),
        'x0': lambda: rdma('x0', u.at[0, 0], u.at[2, 0], px),
        'y0': lambda: rdma('y0', u.at[0, 0], u.at[3, 0], py),
        'x1': lambda: rdma('x1', u.at[0, 1], u.at[2, 1], px),
        'y1': lambda: rdma('y1', u.at[0, 1], u.at[3, 1], py),
        'x2': lambda: rdma('x2', u.at[0, 2], u.at[2, 2], px),
        'y2': lambda: rdma('y2', u.at[0, 2], u.at[3, 2], py),
        'x3': lambda: rdma('x3', u.at[0, 3], u.at[2, 3], px),
        'y3': lambda: rdma('y3', u.at[0, 3], u.at[3, 3], py),
        'd0': lambda: rdma('d0', u.at[2, 0], u.at[6, 0], py),
        'd1': lambda: rdma('d1', u.at[3, 1], u.at[6, 1], px),
        'd2': lambda: rdma('d2', u.at[2, 2], u.at[6, 2], py),
        'd3': lambda: rdma('d3', u.at[3, 3], u.at[6, 3], px),
        'cx0': lambda: rdma('cx0', u.at[2, pl.ds(0, 2)], u.at[4, pl.ds(0, 2)], pc),
        'cx1': lambda: rdma('cx1', u.at[2, pl.ds(2, 2)], u.at[4, pl.ds(2, 2)], pc),
        'cy0': lambda: rdma('cy0', u.at[3, pl.ds(0, 2)], u.at[5, pl.ds(0, 2)], pc),
        'cy1': lambda: rdma('cy1', u.at[3, pl.ds(2, 2)], u.at[5, pl.ds(2, 2)], pc),
        'cd0': lambda: rdma('cd0', u.at[6, pl.ds(0, 2)], u.at[7, pl.ds(0, 2)], pc),
        'cd1': lambda: rdma('cd1', u.at[6, pl.ds(2, 2)], u.at[7, pl.ds(2, 2)], pc),
        'icx': lambda: rdma('icx', info.at[2], info.at[4], pc),
        'icy': lambda: rdma('icy', info.at[3], info.at[5], pc),
        'icd': lambda: rdma('icd', info.at[6], info.at[7], pc),
    }
    for key in ag:
        specs.setdefault(key, len(specs))

    def sums(c, q, half=0):
        return c * 16 + q * 2 + half

    def rs(name, c):
        key = (name, c)
        if name[0] == 'c':
            n = int(name[1])
            return rdma(key, big.at[pl.ds(sums(c, 4 + n), 2)], big.at[pl.ds(RC + c * 8 + n * 2, 2)], pc)
        src, dst, to = {
            'xa': (sums(c, 1, 0), R1 + c * 4, px),
            'xb': (sums(c, 3, 0), R1 + c * 4 + 1, px),
            'ya': (sums(c, 2, 1), R1 + c * 4 + 2, py),
            'yb': (sums(c, 3, 1), R1 + c * 4 + 3, py),
            'y2': (sums(c, 2, 0), R2 + c * 2, py),
            'x2': (sums(c, 1, 1), R2 + c * 2 + 1, px),
        }[name]
        return rdma(key, big.at[src], big.at[dst], to)

    def rs_first(c, qs):
        for q in qs:
            rs('c%d' % q, c).wait_recv()
            for half in range(2):
                k = sums(c, q, half)
                big[k] = big[k] + big[RC + c * 8 + q * 2 + half]
            for name in ((), ('xa',), ('ya',), ('xb', 'yb'))[q]:
                rs(name, c).start()

    def rs_second(c):
        rs('xb', c).wait_recv()
        big[sums(c, 2, 0)] = big[sums(c, 2, 0)] + big[R1 + c * 4 + 1]
        rs('y2', c).start()
        rs('yb', c).wait_recv()
        big[sums(c, 1, 1)] = big[sums(c, 1, 1)] + big[R1 + c * 4 + 3]
        rs('x2', c).start()

    def rs_last(c, f):
        rs('xa', c).wait_recv()
        rs('y2', c).wait_recv()
        m = (big[sums(c, 0, 0)] + big[R1 + c * 4]) + big[R2 + c * 2]
        out[0, :, c * CW:c * CW + HW] = (f[:, :HW] + m).astype(bf16)
        rs('ya', c).wait_recv()
        rs('x2', c).wait_recv()
        m = (big[sums(c, 0, 1)] + big[R1 + c * 4 + 2]) + big[R2 + c * 2 + 1]
        out[0, :, c * CW + HW:(c + 1) * CW] = (f[:, HW:] + m).astype(bf16)

    barrier = pltpu.get_barrier_semaphore()
    for to in (px, py, pc):
        pl.semaphore_signal(barrier, inc=1, device_id=to, device_id_type=MESH)
    loads = [pltpu.make_async_copy(src, dst, sem_in.at[i]) for i, (src, dst) in enumerate((
        (h0_h, h0), (nm_h, nm), (na_h, na), (idx_h, idx), (slot_h, slot), (wr_h, wr), (cos_h, cos), (sin_h, sin),
        (nf_h, nf)))]
    for load in loads:
        load.start()
    for i, src in enumerate((wk, wv)):
        pltpu.make_async_copy(src, ring.at[i, :, pl.ds(0, QT)], sem.at[i]).start()

    for load in loads[:3]:
        load.wait()
    for t in range(T_Q, NS):
        start(t)

    def norms(i, _):
        rows = pl.ds(pl.multiple_of(i * 16, 16), 16)
        xf = h0[0, rows, :].astype(f32)
        xr = xf * lax.rsqrt(jnp.mean(xf * xf, axis=-1, keepdims=True) + EPS)
        un = (xr * nm[...].astype(f32)[None, :]).astype(bf16)
        for k in range(4):
            u[0, k, rows, :] = un[:, k * 512:(k + 1) * 512]
        xz[rows, :] = (xr * na[...].astype(f32)[None, :]).astype(bf16)
        return 0

    lax.fori_loop(0, T // 16, norms, 0, unroll=4)
    pl.semaphore_wait(barrier, 3)
    for key in ('x0', 'y1', 'c0'):
        ag[key]().start()

    for load in loads[3:]:
        load.wait()
    logits = _dot(u[0, 0], wr[pl.ds(0, 512), :])
    for k in range(1, 4):
        logits = logits + _dot(u[0, k], wr[pl.ds(k * 512, 512), :])
    lt = logits.T
    idt = idx[0].astype(f32)
    slt = slot[0].astype(f32)
    ex = lax.broadcasted_iota(jnp.int32, (T, T), 0).astype(f32)
    sel = jnp.concatenate(
        [jnp.sum(jnp.where(ex == idt[j:j + 1, :], lt, 0.0), axis=0, keepdims=True) for j in range(TOP)], axis=0)
    gate = jnp.exp(sel - jnp.max(sel, axis=0, keepdims=True))
    gate = gate / jnp.sum(gate, axis=0, keepdims=True)
    info[0, pl.ds(0, TOP), :] = idt * float(CAP) + slt
    info[0, pl.ds(TOP, TOP), :] = gate
    for key in ('ix', 'iy', 'ic', 'x1', 'y0', 'c1'):
        ag[key]().start()

    cs, sn = cos[...], sin[...]

    def rope(v):
        return (v * cs + pltpu.roll(v, HEAD // 2, 1) * sn).astype(bf16)

    wait(0)
    wait(1)
    kf = _dot(xz[...], ring[0, :, pl.ds(0, QT)])
    vf = _dot(xz[...], ring[1, :, pl.ds(0, QT)])
    for n in range(4):
        kk[n] = rope(kf[:, n * HEAD:(n + 1) * HEAD])
        vv[n] = vf[:, n * HEAD:(n + 1) * HEAD].astype(bf16)
    start(NS)
    start(NS + 1)
    causal = lax.broadcasted_iota(jnp.int32, (T, T), 0) >= lax.broadcasted_iota(jnp.int32, (T, T), 1)

    def q_dot(s, dst):
        dst[...] = _dot(xz[...], ring[s, :, pl.ds(0, QT)])

    def q_heads(i, src):
        kg, vg = kk[i // 2], vv[i // 2]
        qs = jnp.concatenate([rope(src[:, n * HEAD:(n + 1) * HEAD]) for n in range(4)], axis=0)
        sc = lax.dot_general(qs, kg, (((1,), (1,)), ((), ())), preferred_element_type=f32) * HEAD ** -0.5
        ps = []
        for n in range(4):
            sm = jnp.where(causal, sc[n * T:(n + 1) * T], -jnp.inf)
            p = jnp.exp(sm - jnp.max(sm, axis=-1, keepdims=True))
            ps.append((p * (1.0 / jnp.sum(p, axis=-1, keepdims=True))).astype(bf16))
        o = _dot(jnp.concatenate(ps, axis=0), vg)
        for n in range(4):
            g[:, pl.ds(_mult(i * QT) + n * HEAD, HEAD)] = o[n * T:(n + 1) * T].astype(bf16)

    def q_pair(k, _):
        t = T_Q + 2 * k + 1
        s = wait(t), wait(t + 1)
        q_dot(s[0], qb)
        q_heads(2 * k, qa)
        q_dot(s[1], qa)
        q_heads(2 * k + 1, qb)
        start(t + NS, T_WO1, T_E2)
        start(t + 1 + NS, T_WO1, T_E2)

        @pl.when(k == Q_FWD)
        def _():
            ag['ix']().wait_recv()
            ag['id']().start()
            ag['x0']().wait_recv()
            ag['d0']().start()
            ag['y1']().wait_recv()
            ag['d1']().start()
            for key in ('x2', 'y3', 'x3', 'y2'):
                ag[key]().start()

        return 0

    q_dot(wait(T_Q), qa)
    start(T_Q + NS)
    lax.fori_loop(0, NQ // 2 - 1, q_pair, 0)
    s_last = wait(T_WO1 - 1)
    q_dot(s_last, qb)
    q_heads(NQ - 2, qa)
    q_heads(NQ - 1, qb)
    start(T_WO1 - 1 + NS)
    for key in ('iy', 'id', 'x1', 'y0'):
        ag[key]().wait_recv()
    for key in ('icx', 'icy', 'icd', 'cx0', 'cy0'):
        ag[key]().start()

    def wo_step(n, t):
        cols = slice(n * CW, (n + 1) * CW)
        s0, s1 = wait(t), wait(t + 1)
        prod = _dot(g[:, :2048], ring[s0, :, pl.ds(0, CW)])
        start(t + NS)
        prod = prod + _dot(g[:, 2048:4096], ring[s1, :, pl.ds(0, CW)])
        start(t + 1 + NS)
        ar[:, cols] = (h0[0, :, cols].astype(f32) + prod).astype(bf16)

    wo_step(0, T_WO1)

    base = ((ep * 32 + e0) * CAP).astype(f32)

    def weights(r):
        for half in range(2):
            row = lax.broadcasted_iota(jnp.int32, (T, T), 0).astype(f32) + (base + float(half * T))
            w = jnp.zeros((T, T), f32)
            d = jnp.zeros((T, T), f32)
            for j in range(TOP):
                hit = row == info[r, pl.ds(j, 1), :]
                w = jnp.where(hit, info[r, pl.ds(TOP + j, 1), :], w)
                d = jnp.where(hit, 1.0, d)
            wt = w.T
            hi = wt.astype(bf16)
            rest = wt - hi.astype(f32)
            mid = rest.astype(bf16)
            low = (rest - mid.astype(f32)).astype(bf16)
            for n, part in enumerate((hi, mid, low)):
                ws[r, pl.ds(n * T, T), half * T:(half + 1) * T] = part
            ds[r, pl.ds(half * T, T), :] = d.astype(bf16)

    def rows_of(r, k):
        rows = _dot(ds[r], u[r, k]).astype(bf16)
        x[:, pl.ds(pl.multiple_of(r * CAP, CAP), CAP), k * 512:(k + 1) * 512] = rows.reshape(EL, CAP, 512)

    def build(r, _):
        weights(r)
        for k in range(2):
            rows_of(r, k)
        return 0

    for key in ('ic', 'c0'):
        ag[key]().wait_recv()
    lax.fori_loop(0, 4, build, 0)
    for key in ('d0', 'd1'):
        ag[key]().wait_recv()
    ag['cd0']().start()
    for n in range(1, NW):
        wo_step(n, T_WO1 + 2 * n)
    for key in ('icx', 'icy', 'icd', 'cx0', 'cy0'):
        ag[key]().wait_recv()
    lax.fori_loop(4, 7, build, 0)
    ag['cd0']().wait_recv()
    build(7, 0)

    def products(lhs, s):
        ha = _dot(lhs, ring[s, pl.ds(0, KH), :])
        hc = _dot(lhs, ring[s, pl.ds(KH, KH), :])
        return [h[:, j * HW:(j + 1) * HW] for h in (ha, hc) for j in range(3)]

    def first_half(i, _):
        t = T_EXP + 2 * i
        slots = [wait(t + k, width=FE) for k in range(2)]
        for k in range(2):
            e = 2 * i + k
            for j, h in enumerate(products(x[e, :, :KH], slots[k])):
                big[e * 6 + j] = h
            start(t + k + NS, T_EXP + NS, T_E2)

    def first_early(i, _):
        first_half(i, 0)

        @pl.when(i == E_FWD[0])
        def _():
            ag['x2']().wait_recv()
            ag['d2']().start()
            ag['y3']().wait_recv()
            ag['d3']().start()

        @pl.when(i == E_FWD[1])
        def _():
            for key in ('x3', 'y2'):
                ag[key]().wait_recv()
            for key in ('cx1', 'cy1'):
                ag[key]().start()

        @pl.when(i == E_FWD[2])
        def _():
            for key in ('d2', 'd3'):
                ag[key]().wait_recv()
            ag['cd1']().start()
        return 0

    def first_late(i, _):
        first_half(i, 0)
        for k in range(2, 4):
            for j in range(4):
                rows_of(4 * (i - EARLY) + j, k)
        return 0

    lax.fori_loop(0, EARLY, first_early, 0)
    for key in ('c1', 'cx1', 'cy1', 'cd1'):
        ag[key]().wait_recv()
    lax.fori_loop(EARLY, 8, first_late, 0)

    def second_half(lo, hi):
        def step(i, _):
            t = T_EXP + EL + 2 * i
            slots = [wait(t + k, width=FE) for k in range(2)]
            for k in range(2):
                e = EL - 1 - (2 * i + k)
                hs = [h + big[e * 6 + j] for j, h in enumerate(products(x[e, :, KH:], slots[k]))]
                start(t + k + NS, lo, hi)
                for j in range(3):
                    x[e, :, j * HW:(j + 1) * HW] = (hs[j] * jax.nn.sigmoid(hs[j]) * hs[3 + j]).astype(bf16)
            return 0
        return step

    turn = (EL - NS) // 2
    lax.fori_loop(0, turn, second_half(T_EXP + EL + NS, T_E2), 0)
    if (EL - NS) % 2:
        second_half(0, T_END)(turn, 0)
        turn += 1
    lax.fori_loop(turn, EL // 2, second_half(T_E2, T_WO), 0)
    pl.semaphore_signal(ready, inc=1, device_id=pc, device_id_type=MESH)

    YC = 1024

    def chunk(c):
        def part(k):
            t = T_E2 + 8 * c + 4 * k
            slots = [wait(t + j, E2) for j in range(4)]
            for j in range(4):
                for i in range(2):
                    e = 8 * k + 2 * j + i
                    x[e, :, YC:YC + CW] = _dot(x[e, :, :FE], ring[slots[j], pl.ds(i * FE, FE), pl.ds(0, CW)]).astype(bf16)
                start(t + j + NS)

        part(0)
        if c > 0:
            rs_first(c - 1, (1, 2, 0))
        part(1)
        if c == 0:
            pl.semaphore_wait(ready, 1)
        if c == 2:
            rs_second(0)

        for q in (7, 3, 5, 6, 4, 1, 2, 0):
            if c == 0 and q == 2:
                rs_first(c, (3,))
            r = PLACE[q]
            yr = x[:, r * CAP:(r + 1) * CAP, YC:YC + CW].reshape(2 * T, CW)
            three = _dot(ws[r], yr)
            m = (three[:T] + three[T:2 * T]) + three[2 * T:]
            big[sums(c, q, 0)] = m[:, :HW]
            big[sums(c, q, 1)] = m[:, HW:]
            if q >= 4:
                rs('c%d' % (q - 4), c).start()
        if c > 0:
            rs_first(c, (3,))

    for c in range(NC):
        chunk(c)

    for n in range(NW, NC):
        wo_step(n, T_WO + 2 * (n - NW))
        if n == NW:
            rs_first(NC - 1, (1, 2, 0))
            rs_second(1)

    def znorm(i, _):
        rows = pl.ds(pl.multiple_of(i * 16, 16), 16)
        xf = ar[rows, :].astype(f32)
        xr = xf * lax.rsqrt(jnp.mean(xf * xf, axis=-1, keepdims=True) + EPS)
        xz[rows, :] = (xr * nf[...].astype(f32)[None, :]).astype(bf16)
        return 0

    lax.fori_loop(0, T // 16, znorm, 0, unroll=4)

    def ffn(lo, hi):
        def step(i, _):
            t = T_FFN + 4 * i
            slots = [wait(t + k, width=FE) for k in range(4)]
            for k in range(2):
                h1 = _dot(xz[...], ring[slots[2 * k]])
                start(t + 2 * k + NS, lo, hi, NS % 2)
                h3 = _dot(xz[...], ring[slots[2 * k + 1]])
                start(t + 2 * k + 1 + NS, lo, hi, (NS + 1) % 2)
                g[:, pl.ds(_mult(i * 2 * FE) + k * FE, FE)] = (h1 * jax.nn.sigmoid(h1) * h3).astype(bf16)
            return 0
        return step

    turn = (2 * NF - NS) // 4
    lax.fori_loop(0, turn, ffn(T_FFN + NS, T_W2), 0)
    rs_second(2)
    if (2 * NF - NS) % 4:
        ffn(0, T_END)(turn, 0)
        turn += 1
    lax.fori_loop(turn, NF // 2, ffn(T_W2, T_END), 0)
    rs_second(3)

    for n in range(D // CW):
        cols = slice(n * CW, (n + 1) * CW)
        t = T_W2 + 3 * n
        batch = n < NC - 1
        slots = [wait(t + k) for k in range(3)] if batch else None
        prod = None
        for k in range(3):
            s = slots[k] if batch else wait(t + k)
            term = _dot(g[:, k * 2048:(k + 1) * 2048], ring[s, :, pl.ds(0, CW)])
            prod = term if prod is None else prod + term
            start(t + k + NS, T_W2, T_END)
        if n == 0:
            fs[...] = ar[:, cols].astype(f32) + prod
            continue
        if n == 1:
            rs_last(0, fs[...])
        rs_last(n, ar[:, cols].astype(f32) + prod)

    for key in ag:
        ag[key]().wait_send()
    for c in range(NC):
        for name in ('c0', 'c1', 'c2', 'c3', 'xa', 'xb', 'ya', 'yb', 'y2', 'x2'):
            rs(name, c).wait_send()


def solution(mesh):
    ang = (np.arange(T, dtype=np.float32)[:, None]
           * (ROPE_BASE ** (-2.0 * np.arange(HEAD // 2) / HEAD)).astype(np.float32)[None, :])
    cos = np.cos(ang.astype(np.float64)).astype(np.float32)
    sin = np.sin(ang.astype(np.float64)).astype(np.float32)
    cos2 = np.concatenate([cos, cos], axis=1)
    sin2 = np.concatenate([-sin, sin], axis=1)
    ncopies = 27 + 10 * NC

    def local(h0, idx, slot, na, wq, wk, wv, wo, nf, w1, w3, w2, nm, wr, ue1, ue3, ue2):
        hb = pl.BlockSpec(memory_space=pl.ANY)
        return pl.pallas_call(
            _kernel,
            out_shape=pltpu.VMEM(h0.shape, bf16),
            in_specs=[hb] * 19,
            out_specs=pl.BlockSpec(memory_space=pltpu.VMEM),
            scratch_shapes=[
                pltpu.VMEM(h0.shape, bf16),
                pltpu.VMEM((1, TOP, T), jnp.int32),
                pltpu.VMEM((1, TOP, T), jnp.int32),
                pltpu.VMEM((D,), bf16),
                pltpu.VMEM((D,), bf16),
                pltpu.VMEM((D,), bf16),
                pltpu.VMEM((T, HEAD), f32),
                pltpu.VMEM((T, HEAD), f32),
                pltpu.VMEM(wr.shape, bf16),
                pltpu.SemaphoreType.DMA((9,)),
                pltpu.VMEM((T, D), bf16),
                pltpu.VMEM((T, D), bf16),
                pltpu.VMEM((T, CW), f32),
                pltpu.VMEM((T, QT), f32),
                pltpu.VMEM((T, QT), f32),
                pltpu.VMEM((8, 4, T, D // 4), bf16),
                pltpu.VMEM((8, 2 * TOP, T), f32),
                pltpu.VMEM((8, 3 * T, 2 * T), bf16),
                pltpu.VMEM((8, 2 * T, T), bf16),
                pltpu.VMEM((EL, T, D), bf16),
                pltpu.VMEM((4, T, HEAD), bf16),
                pltpu.VMEM((4, T, HEAD), bf16),
                pltpu.VMEM((T, FF), bf16),
                pltpu.VMEM((NBLK, T, HW), f32),
                pltpu.VMEM((NS, 2048, FE), bf16),
                pltpu.SemaphoreType.DMA((NS,)),
                pltpu.SemaphoreType.DMA((ncopies,)),
                pltpu.SemaphoreType.DMA((ncopies,)),
                pltpu.SemaphoreType.REGULAR,
            ],
            compiler_params=pltpu.CompilerParams(collective_id=0, has_side_effects=True,
                                                 vmem_limit_bytes=66100000),
            name='scmoe',
        )(h0, jnp.swapaxes(idx, 1, 2), jnp.swapaxes(slot, 1, 2), na, nf, nm,
          jnp.asarray(cos2), jnp.asarray(sin2), wr, wq, wk, wv, wo, w1, w3, w2, ue1, ue3, ue2.reshape(-1, D))

    rows = P(('dp', 'ep'))
    in_specs = (rows,) * 3 + (P(),) * 11 + (P('ep'),) * 3
    return jax.shard_map(local, mesh=mesh, in_specs=in_specs, out_specs=rows, check_vma=False)
```
